32 devices in a mesh: row: 8 (over y, x, core), col: 4 (over z).
Axes of the slice: x: 2, y: 2, z: 4, core: 2. Of those that a mesh axis runs over, the one named last changes fastest.
Arguments:
- features: bfloat16 [65536, 256], P(('row', 'col')), may hold values from -6 to 6
- tiles: bfloat16 [8, 4, 768, 128, 128], P('row', 'col'), as said below
- tile_rows: int32 [8, 4, 768], P('row', 'col'), may hold values from 0 to 63
- tile_cols: int32 [8, 4, 768], P('row', 'col'), may hold values from 0 to 127
- valid: int32 [8, 4, 768], P('row', 'col'), may hold values from 0 to 1, as said below
- weight: bfloat16 [256, 256], replicated, may hold values from -0.375 to 0.375
- bias: float32 [256], replicated, may hold values from -3 to 3
Outputs:
- hidden: bfloat16 [65536, 256], P(('row', 'col'))
The draws below stay inside these ranges and needn't reach their ends.
Inputs may be any that keep to these rules, and one draw needn't show every extreme that they name: Each cell holds between 96 and 384 valid slots at any positions; in every draw some cell has exactly 384 valid slots. `tiles`: tile entries are non-negative.
All inputs are finite; a program needn't handle non-finite values.
Results may differ from the reference program's by a relative error of at most 0.0039.
Values may be sent and summed in bfloat16 or wider, within the bound.
A program may use at most 256 MiB of HBM per device.

```python
import jax
import jax.numpy as jnp
from jax import lax

F = 256
TILE = 128
SUB = 2048
TPD = 768
NODES = 65536
N_ROW = 8
N_COL = 4


def draw_tiles(key, part):
    shape = (N_ROW, N_COL, TPD, TILE, TILE)
    spread = (SUB / (TPD * TILE * TILE)) ** 0.5
    values = jnp.minimum(jnp.abs(jax.random.normal(key, shape, jnp.float32)) * spread, 5.0 * spread)
    return values.astype(jnp.bfloat16)


def draw_valid(key, part):
    subkeys = jax.random.split(key, 3)
    cells = N_ROW * N_COL
    shifts = jax.random.randint(subkeys[0], (cells,), 1, 4)
    counts = jnp.right_shift(jnp.full((cells,), TPD, jnp.int32), shifts)
    chosen = jax.random.randint(subkeys[1], (), 0, cells)
    counts = jnp.where(jnp.arange(cells) == chosen, TPD // 2, counts)
    orders = jax.vmap(lambda sub_key: jax.random.permutation(sub_key, TPD))(jax.random.split(subkeys[2], cells))
    valid_flags = (orders < counts[:, None]).astype(jnp.int32)
    return valid_flags.reshape(N_ROW, N_COL, TPD)


def touch_ends(values, own_key, smallest, high):
    shape = values.shape
    index_at = [jax.random.randint(jax.random.fold_in(own_key, axis), (), 0, shape[axis]) for axis in range(len(shape))]
    values = values.at[tuple(index_at)].set(smallest)
    longest = shape.index(max(shape))
    index_at[longest] = (index_at[longest] + 1) % shape[longest]
    return values.at[tuple(index_at)].set(high)


def block_scale(rng, dims, cuts, least, high):
    factor_of, own = 1.0, jax.random.fold_in(rng, 6)
    for dim, shards_of in cuts:
        heights = jnp.exp(jax.random.uniform(jax.random.fold_in(own, dim), (shards_of,), jnp.float32, least / len(cuts), high / len(cuts)))
        factor_of = factor_of * jnp.repeat(heights, dims[dim] // shards_of).reshape([-1 if axis == dim else 1 for axis in range(len(dims))])
    return factor_of


def gaussian(key, extent, scale, limit, pieces=(), kind=jnp.bfloat16):
    entries = jax.random.normal(key, extent, jnp.float32) * scale
    if len(pieces) > 0:
        entries = block_scale(key, extent, pieces, -0.22, 0.18) * entries
    return jnp.clip(entries, min=-limit, max=limit).astype(kind)


def setup_inputs(seed: int = 0) -> dict:
    key_list = jax.random.split(jax.random.key(seed), 8)
    features = gaussian(key_list[0], (NODES, F), 1.0, 6.0, ((0, 32),))
    tiles = draw_tiles(jax.random.fold_in(key_list[7], 71), 0)
    tile_rows = touch_ends(jax.random.randint(key_list[2], (N_ROW, N_COL, TPD), 0, SUB * N_COL // TILE), jax.random.fold_in(key_list[2], 1), 0, (SUB * N_COL // TILE) - 1).astype(jnp.int32)
    tile_cols = touch_ends(jax.random.randint(key_list[3], (N_ROW, N_COL, TPD), 0, SUB * N_ROW // TILE), jax.random.fold_in(key_list[3], 1), 0, (SUB * N_ROW // TILE) - 1).astype(jnp.int32)
    valid = draw_valid(jax.random.fold_in(key_list[7], 71), 0)
    weight = gaussian(key_list[5], (F, F), F ** -0.5, 0.375)
    bias = gaussian(key_list[6], (F,), 0.5, 3.0, (), jnp.float32)
    return {"features": features, "tiles": tiles, "tile_rows": tile_rows, "tile_cols": tile_cols, "valid": valid, "weight": weight, "bias": bias}


def reference(features, tiles, tile_rows, tile_cols, valid, weight, bias):
    row_tiles = SUB * N_COL // TILE
    grouped = features.reshape(N_ROW, N_COL, SUB, F)
    flat_tiles = tiles.reshape(N_ROW * N_COL, TPD, TILE, TILE)
    flat_rows = tile_rows.reshape(N_ROW * N_COL, TPD)
    flat_cols = tile_cols.reshape(N_ROW * N_COL, TPD)
    flat_valid = valid.reshape(N_ROW * N_COL, TPD)

    def one_cell(device):
        column = device % N_COL
        panel = jnp.take(grouped, column, axis=1).reshape(-1, TILE, F)
        chosen = panel[flat_cols[device]]
        products = jnp.einsum("bij,bjf->bif", flat_tiles[device].astype(jnp.float32), chosen.astype(jnp.float32))
        products = products * flat_valid[device].astype(jnp.float32)[:, None, None]
        partial_sum = jnp.zeros((row_tiles, TILE, F), jnp.float32)
        return partial_sum.at[flat_rows[device]].add(products)

    partials = lax.map(one_cell, jnp.arange(N_ROW * N_COL, dtype=jnp.int32))
    totals = jnp.sum(partials.reshape(N_ROW, N_COL, row_tiles, TILE, F), axis=1)
    aggregated = totals.reshape(N_ROW * N_COL * SUB, F).astype(jnp.bfloat16)
    mixed = jnp.dot(aggregated, weight, preferred_element_type=jnp.float32) + bias
    return jnp.maximum(mixed, 0.0).astype(jnp.bfloat16)
```

```python
import functools

import jax
import jax.numpy as jnp
from jax import lax
from jax.experimental import pallas as pl
from jax.experimental.pallas import tpu as pltpu
from jax.sharding import PartitionSpec as P

SLOTS = 32
UNROLL = 8


def spmm_kernel(valid, rows, cols, panel_hbm, tiles_hbm, total,
                slot_list, row_list, col_list, panel, ring, ring_sem, panel_sem):
    slot_count = valid.shape[2]
    row_tiles = total.shape[0] - 1
    panel_copy = pltpu.make_async_copy(panel_hbm, panel, panel_sem)
    panel_copy.start()

    def scan(step, count):
        for k in range(UNROLL):
            slot = step * UNROLL + k
            slot_list[count] = slot
            row_list[count] = rows[0, 0, slot]
            col_list[count] = cols[0, 0, slot]
            count = count + valid[0, 0, slot]
        return count

    count = lax.fori_loop(0, slot_count // UNROLL, scan, jnp.int32(0))
    for k in range(UNROLL):
        slot_list[count + k] = 0
        row_list[count + k] = row_tiles
        col_list[count + k] = 0
    steps = (count + UNROLL - 1) // UNROLL
    filled = steps * UNROLL

    def fetch(index):
        place = lax.rem(index, SLOTS)
        return pltpu.make_async_copy(
            tiles_hbm.at[0, 0, slot_list[index]], ring.at[place], ring_sem.at[place])

    def prime(index, carry):
        @pl.when(index < filled)
        def _():
            fetch(index).start()
        return carry

    lax.fori_loop(0, SLOTS, prime, 0)
    total[...] = jnp.zeros_like(total)
    panel_copy.wait()

    def step_body(step, carry):
        base = step * UNROLL
        for k in range(UNROLL):
            fetch(base + k).wait()
        for k in range(UNROLL):
            index = base + k
            product = jnp.dot(ring[lax.rem(index, SLOTS)], panel[col_list[index]],
                              preferred_element_type=jnp.float32)
            row = row_list[index]
            total[row] = total[row] + product
        for k in range(UNROLL):
            later = base + SLOTS + k

            @pl.when(later < filled)
            def _():
                fetch(later).start()
        return carry

    lax.fori_loop(0, steps, step_body, 0)


def spmm(valid, rows, cols, panel, tiles, row_tiles):
    slot_count, tile_size = tiles.shape[2], tiles.shape[3]
    width = panel.shape[2]
    smem = pl.BlockSpec(memory_space=pltpu.SMEM)
    hbm = pl.BlockSpec(memory_space=pl.ANY)
    return pl.pallas_call(
        spmm_kernel,
        out_shape=jax.ShapeDtypeStruct((row_tiles + 1, tile_size, width), jnp.float32),
        in_specs=[smem, smem, smem, hbm, hbm],
        out_specs=pl.BlockSpec(memory_space=pltpu.VMEM),
        scratch_shapes=[
            pltpu.SMEM((slot_count + UNROLL,), jnp.int32),
            pltpu.SMEM((slot_count + UNROLL,), jnp.int32),
            pltpu.SMEM((slot_count + UNROLL,), jnp.int32),
            pltpu.VMEM(panel.shape, jnp.bfloat16),
            pltpu.VMEM((SLOTS, tile_size, tile_size), jnp.bfloat16),
            pltpu.SemaphoreType.DMA((SLOTS,)),
            pltpu.SemaphoreType.DMA,
        ],
        compiler_params=pltpu.CompilerParams(vmem_limit_bytes=60 * 2**20),
        cost_estimate=pl.CostEstimate(
            flops=slot_count * tile_size * tile_size * width, bytes_accessed=32 * 2**20,
            transcendentals=0),
    )(valid, rows, cols, panel, tiles)


MESH = pl.DeviceIdType.MESH
PIECES = 2


def gather_steps(features, lane, panel, send_sem, recv_sem, local_sem, rows):
    sub_rows, width = panel.shape[1], panel.shape[2]
    cut = sub_rows // 2
    me = lax.axis_index("row")
    chips = rows // 2
    core, chip = lax.rem(me, 2), me // 2
    partner = chip * 2 + (1 - core)
    own = features.at[:, pl.ds(lane * width, width)]

    def half(ref, k):
        return ref.at[pl.ds(k * cut, cut)]

    def copy(src, block, k, number, target):
        return pltpu.make_async_remote_copy(
            src_ref=src, dst_ref=half(panel.at[block], k), send_sem=send_sem.at[number],
            recv_sem=recv_sem.at[number], device_id={"row": target}, device_id_type=MESH)

    def held(block, k):
        return half(panel.at[block], k)

    if chips == 4:
        over_x, over_y = lax.rem(chip, 2), chip // 2
        x_side = (over_y * 2 + (1 - over_x)) * 2 + core
        y_side = ((1 - over_y) * 2 + over_x) * 2 + core
        across = ((1 - over_y) * 2 + (1 - over_x)) * 2 + core
        peers = [x_side, y_side]
        sources = [x_side, y_side, y_side, x_side]
        own_copies = [copy(half(own, 0), me, 0, 0, x_side), copy(half(own, 1), me, 1, 1, y_side),
                      copy(half(own, 1), me, 1, 2, x_side), copy(half(own, 0), me, 0, 3, y_side)]
        passed = {0: copy(held(x_side, 0), x_side, 0, 4, y_side),
                  1: copy(held(y_side, 1), y_side, 1, 5, x_side)}
        arriving = [(x_side, 0), (y_side, 1), (x_side, 1), (y_side, 0), (across, 0), (across, 1)]
    else:
        peers = [lax.rem(chip + k, chips) * 2 + core for k in range(1, chips)]
        from_peers = [lax.rem(chip + chips - k, chips) * 2 + core for k in range(1, chips)]
        own_copies, passed, arriving = [], {}, []
        for place, (peer, giver) in enumerate(zip(peers, from_peers)):
            for k in range(2):
                own_copies.append(copy(half(own, k), me, k, 2 * place + k, peer))
                arriving.append((giver, k))
    direct = len(arriving)
    started = list(own_copies)
    keep = pltpu.make_async_copy(own, panel.at[me], local_sem)

    def begin():
        for item in own_copies:
            item.start()
        for k in range(2):
            item = copy(half(own, k), me, k, direct + k, partner)
            item.start()
            started.append(item)
        keep.start()

    def receive(number):
        block, k = arriving[number]
        copy(held(block, k), block, k, number, partner).wait_recv()
        if number in passed:
            passed[number].start()
            started.append(passed[number])
        item = copy(held(block, k), block, k, direct + 2 + number, partner)
        item.start()
        started.append(item)

    def finish():
        for number in range(direct + 2):
            copy(held(me, 0), me, 0, direct + number, partner).wait_recv()
        for item in started:
            item.wait_send()
        keep.wait()

    steps = [functools.partial(receive, number) for number in range(direct)]
    return peers + [partner], begin, steps, finish


def reduce_steps(partial, summed, to_right, to_left, from_left, from_right, total, sems, columns):
    tiles_each = summed.shape[0]
    cut = tiles_each // PIECES
    me = lax.axis_index("col")
    right_send, right_recv, left_send, left_recv = sems

    def move(rightward, dest, piece):
        place = dest - 1 if rightward else dest
        outbox, inbox = (to_right, from_left) if rightward else (to_left, from_right)
        send, recv = (right_send, right_recv) if rightward else (left_send, left_recv)
        part = pl.ds(piece * cut, cut)
        inner = (me < dest) if rightward else (me > dest)
        first = (me == 0) if rightward else (me == columns - 1)
        number = place * PIECES + piece
        target = me + 1 if rightward else me - 1
        item = pltpu.make_async_remote_copy(
            src_ref=outbox.at[place, part], dst_ref=inbox.at[place, part],
            send_sem=send.at[number], recv_sem=recv.at[number],
            device_id={"col": target}, device_id_type=MESH)
        here = pl.ds(dest * tiles_each + piece * cut, cut)

        def open_chain():
            @pl.when(first)
            def _():
                outbox[place, part] = partial[here].astype(outbox.dtype)
                item.start()

        def pass_on():
            @pl.when(jnp.logical_and(inner, jnp.logical_not(first)))
            def _():
                item.wait_recv()
                outbox[place, part] = (
                    partial[here] + inbox[place, part].astype(jnp.float32)).astype(outbox.dtype)
                item.start()

        def close_chain():
            @pl.when(me == dest)
            def _():
                item.wait_recv()
                total[part] = total[part] + inbox[place, part].astype(jnp.float32)

        def drain():
            @pl.when(inner)
            def _():
                item.wait_send()

        return open_chain, pass_on, close_chain, drain

    links = []
    for turn in range(columns - 1):
        for piece in range(PIECES):
            links.append(move(True, columns - 1 - turn, piece))
            links.append(move(False, turn, piece))

    def begin():
        for link in links:
            link[0]()
        total[...] = partial[pl.ds(me * tiles_each, tiles_each)]

    def finish():
        for link in links:
            link[2]()
        summed[...] = total[...].astype(summed.dtype)
        for link in links:
            link[3]()

    return begin, [link[1] for link in links], finish


def exchange_kernel(gathering, reducing, lane, rows, columns, *refs):
    refs = list(refs)
    features = refs.pop(0) if gathering else None
    partial = refs.pop(0) if reducing else None
    panel = refs.pop(0) if gathering else None
    summed = refs.pop(0) if reducing else None
    peers, queue = [], []
    if gathering:
        send_sem, recv_sem, local_sem = refs.pop(0), refs.pop(0), refs.pop(0)
        peers, gather_begin, gather_list, gather_finish = gather_steps(
            features, lane, panel, send_sem, recv_sem, local_sem, rows)
    if reducing:
        reduce_begin, reduce_list, reduce_finish = reduce_steps(
            partial, summed, *refs[:5], refs[5:9], columns)

    barrier = pltpu.get_barrier_semaphore()
    for peer in peers:
        pl.semaphore_signal(barrier, inc=1, device_id={"row": peer}, device_id_type=MESH)
    expected = len(peers)
    if reducing:
        me = lax.axis_index("col")

        @pl.when(me > 0)
        def _():
            pl.semaphore_signal(barrier, inc=1, device_id={"col": me - 1}, device_id_type=MESH)

        @pl.when(me < columns - 1)
        def _():
            pl.semaphore_signal(barrier, inc=1, device_id={"col": me + 1}, device_id_type=MESH)

        inside = jnp.logical_and(me > 0, me < columns - 1)

        @pl.when(inside)
        def _():
            pl.semaphore_wait(barrier, expected + 2)

        @pl.when(jnp.logical_not(inside))
        def _():
            pl.semaphore_wait(barrier, expected + 1)
    else:
        pl.semaphore_wait(barrier, expected)

    if gathering:
        gather_begin()
    if reducing:
        reduce_begin()
    gather_queue = list(gather_list) if gathering else []
    reduce_queue = list(reduce_list) if reducing else []
    while gather_queue or reduce_queue:
        for queue in (gather_queue, reduce_queue):
            for _ in range(2):
                if queue:
                    queue.pop(0)()
    if gathering:
        gather_finish()
    if reducing:
        reduce_finish()


def exchange(number, features, lane, partial, width, tile_size, rows, columns):
    gathering, reducing = features is not None, partial is not None
    hbm, vmem = pl.BlockSpec(memory_space=pl.ANY), pl.BlockSpec(memory_space=pltpu.VMEM)
    operands, in_specs, out_shape, out_specs, scratch = [], [], [], [], []
    if gathering:
        sub_rows = features.shape[0]
        operands.append(features)
        in_specs.append(hbm)
        out_shape.append(jax.ShapeDtypeStruct((rows, sub_rows, width), jnp.bfloat16))
        out_specs.append(hbm)
        chips = rows // 2
        copies = 2 * (6 if chips == 4 else 2 * (chips - 1)) + 2
        scratch += [pltpu.SemaphoreType.DMA((copies,)), pltpu.SemaphoreType.DMA((copies,)),
                    pltpu.SemaphoreType.DMA]
    if reducing:
        tiles_each = (partial.shape[0] - 1) // columns
        operands.append(partial)
        in_specs.append(vmem)
        out_shape.append(jax.ShapeDtypeStruct((tiles_each, tile_size, width), jnp.bfloat16))
        out_specs.append(vmem)
        scratch += [pltpu.VMEM((columns - 1, tiles_each, tile_size, width), jnp.bfloat16)] * 4
        scratch += [pltpu.VMEM((tiles_each, tile_size, width), jnp.float32)]
        scratch += [pltpu.SemaphoreType.DMA(((columns - 1) * PIECES,))] * 4
    return pl.pallas_call(
        functools.partial(exchange_kernel, gathering, reducing, lane, rows, columns),
        out_shape=out_shape, in_specs=in_specs, out_specs=out_specs, scratch_shapes=scratch,
        compiler_params=pltpu.CompilerParams(
            collective_id=number, has_side_effects=True, vmem_limit_bytes=60 * 2**20),
    )(*operands)


LANES = 128
FIELD_BITS = 10
FIELD = 2**FIELD_BITS
FIRST = FIELD * FIELD
PAIR_UNROLL = 16
CUTS = 4
TILE_COPIES = 8
VMEM_ROOM = 63 * 2**20


def wanted_order(rows_v, cols_v, valid_v, codes_v, lasts_v, pairs):
    slot_count = rows_v.shape[2]
    lane = lax.broadcasted_iota(jnp.int32, (1, LANES), 1)
    tall = lax.broadcasted_iota(jnp.int32, (LANES, LANES), 0)
    tall_slots = lax.broadcasted_iota(jnp.int32, (slot_count, LANES), 0)
    chunks = slot_count // LANES

    def upright(pieces):
        turned = [jnp.broadcast_to(piece, (LANES, LANES)).T for piece in pieces]
        return turned[0] if len(turned) == 1 else jnp.concatenate(turned, axis=0)

    def tally(hits, amounts):
        return jnp.sum(jnp.where(hits, amounts, 0), axis=0, keepdims=True)

    keys, columns_of = [], []
    for chunk in range(chunks):
        part = pl.ds(chunk * LANES, LANES)
        keys.append(jnp.where(valid_v[0, :, part] > 0, rows_v[0, :, part], -1))
        columns_of.append(cols_v[0, :, part])
    key_tall = upright(keys)
    held = tally(key_tall == lane, 1)
    halves = lax.shift_right_logical(held + 1, 1)
    halves_tall = upright([halves])
    lasts_v[...] = jnp.where(
        held > 0, tally(tall < lane, halves_tall) + halves - 1, pairs)
    places, codes = [], []
    for chunk in range(chunks):
        slot = lane + chunk * LANES
        before = tally(jnp.logical_and(key_tall == keys[chunk], tall_slots < slot), 1)
        start = tally(tall < keys[chunk], halves_tall)
        places.append(jnp.where(keys[chunk] >= 0, 2 * start + before, -1))
        codes.append(slot - slot_count + columns_of[chunk] * FIELD
                     + jnp.where(before == 0, FIRST, 0))
    place_tall, code_tall = upright(places), upright(codes)
    for chunk in range(codes_v.shape[1] // LANES):
        found = tally(place_tall == lane + chunk * LANES, code_tall)
        codes_v[:, pl.ds(chunk * LANES, LANES)] = found + slot_count


def multiply(codes, tiles, panel, prefix, pairs):
    def operands(code):
        column = jnp.bitwise_and(lax.shift_right_logical(code, FIELD_BITS), FIELD - 1)
        return tiles[jnp.bitwise_and(code, FIELD - 1)], panel[column]

    def body(step, total):
        for k in range(PAIR_UNROLL):
            pair = step * PAIR_UNROLL + k
            code = codes[0, 2 * pair]
            left, upper = operands(code)
            right, lower = operands(codes[0, 2 * pair + 1])
            product = jnp.dot(jnp.concatenate([left, right], axis=1),
                              jnp.concatenate([upper, lower], axis=0),
                              preferred_element_type=jnp.float32)
            opens = jnp.full(total.shape, code, jnp.int32) >= FIRST
            total = jnp.where(opens, 0.0, total) + product
            prefix[pair] = total
        return total

    lax.fori_loop(0, pairs // PAIR_UNROLL, body, jnp.zeros(panel.shape[1:], jnp.float32))


def gather_lane(panel, send_sem, recv_sem, sub_tiles):
    cut = sub_tiles // 2
    me = lax.axis_index("row")
    core, chip = lax.rem(me, 2), me // 2
    partner = chip * 2 + (1 - core)
    over_x, over_y = lax.rem(chip, 2), chip // 2
    x_side = (over_y * 2 + (1 - over_x)) * 2 + core
    y_side = ((1 - over_y) * 2 + over_x) * 2 + core
    across = ((1 - over_y) * 2 + (1 - over_x)) * 2 + core

    def copy(block, k, number, target):
        part = panel.at[pl.ds(block * sub_tiles + k * cut, cut)]
        return pltpu.make_async_remote_copy(
            src_ref=part, dst_ref=part, send_sem=send_sem.at[number],
            recv_sem=recv_sem.at[number], device_id={"row": target}, device_id_type=MESH)

    own = [copy(me, 0, 0, x_side), copy(me, 1, 1, y_side),
           copy(me, 1, 2, x_side), copy(me, 0, 3, y_side)]
    passed = {0: copy(x_side, 0, 4, y_side), 1: copy(y_side, 1, 5, x_side)}
    arriving = [(x_side, 0), (y_side, 1), (x_side, 1), (y_side, 0), (across, 0), (across, 1)]
    direct = len(arriving)
    started = []

    def start(item):
        item.start()
        started.append(item)

    def begin():
        for item in own:
            start(item)
        for k in range(2):
            start(copy(me, k, direct + k, partner))

    def receive(number):
        block, k = arriving[number]
        copy(block, k, number, partner).wait_recv()
        if number in passed:
            start(passed[number])
        start(copy(block, k, direct + 2 + number, partner))

    def finish():
        for number in range(direct + 2):
            copy(me, 0, direct + number, partner).wait_recv()

    def drain():
        for item in started:
            item.wait_send()

    return [x_side, y_side, partner], begin, receive, finish, drain


def reduce_lane(prefix, lasts, partial, boxes, sems, columns):
    tiles_each = boxes.shape[1]
    cut = tiles_each // CUTS
    me = lax.axis_index("col")
    ends = jnp.logical_or(me == 0, me == columns - 1)
    send, recv = sems

    def link(rightward, dest, piece):
        part = pl.ds(piece * cut, cut)
        place = dest - 1 if rightward else dest
        number = ((0 if rightward else 1) * (columns - 1) + place) * CUTS + piece
        target = me + 1 if rightward else me - 1
        here = dest - me if rightward else columns - me + dest
        there = here - 1 if rightward else here + 1
        inner = (me < dest) if rightward else (me > dest)
        first = (me == 0) if rightward else (me == columns - 1)

        def outgoing():
            return pltpu.make_async_remote_copy(
                src_ref=boxes.at[here, part], dst_ref=boxes.at[there, part],
                send_sem=send.at[number], recv_sem=recv.at[number],
                device_id={"col": target}, device_id_type=MESH)

        def incoming():
            return pltpu.make_async_remote_copy(
                src_ref=boxes.at[here, part], dst_ref=boxes.at[here, part],
                send_sem=send.at[number], recv_sem=recv.at[number],
                device_id={"col": target}, device_id_type=MESH)

        def open_chain():
            @pl.when(first)
            def _():
                def body(k, carry):
                    tile = piece * cut + k
                    boxes[here, tile] = prefix[lasts[0, dest * tiles_each + tile]].astype(boxes.dtype)
                    return carry
                lax.fori_loop(0, cut, body, 0)
                outgoing().start()

        def pass_on():
            @pl.when(jnp.logical_and(inner, jnp.logical_not(first)))
            def _():
                incoming().wait_recv()

                def body(k, carry):
                    tile = piece * cut + k
                    boxes[here, tile] = (
                        partial[dest * tiles_each + tile]
                        + boxes[here, tile].astype(jnp.float32)).astype(boxes.dtype)
                    return carry
                lax.fori_loop(0, cut, body, 0)
                outgoing().start()

        def close_chain():
            @pl.when(jnp.logical_and(me == dest, jnp.logical_not(first)))
            def _():
                incoming().wait_recv()

                def body(k, carry):
                    tile = piece * cut + k
                    own = dest * tiles_each + tile
                    partial[own] = partial[own] + boxes[here, tile].astype(jnp.float32)
                    return carry
                lax.fori_loop(0, cut, body, 0)

        def drain():
            @pl.when(inner)
            def _():
                outgoing().wait_send()

        return open_chain, pass_on, close_chain, drain

    links = []
    for turn in range(columns - 1):
        for piece in range(CUTS):
            links.append(link(True, columns - 1 - turn, piece))
            links.append(link(False, turn, piece))

    def begin():
        for item in links:
            item[0]()

        @pl.when(jnp.logical_not(ends))
        def _():
            def body(tile, carry):
                partial[tile] = prefix[lasts[0, tile]]
                return carry
            lax.fori_loop(0, columns * tiles_each, body, 0)

        @pl.when(ends)
        def _():
            def body(k, carry):
                tile = me * tiles_each + k
                partial[tile] = prefix[lasts[0, tile]]
                return carry
            lax.fori_loop(0, tiles_each, body, 0)

    passes = [item[1] for item in links]

    def close(piece):
        for dest in range(columns):
            if dest > 0:
                link(True, dest, piece)[2]()
            if dest < columns - 1:
                link(False, dest, piece)[2]()

    def drain():
        for item in links:
            item[3]()

    return begin, passes, close, drain


def layer_kernel(rows, columns, pairs, features, tiles_hbm, tile_rows, tile_cols, valid, weight_hbm,
                 bias_hbm, out, tiles, prefix, rows_v, cols_v, valid_v, codes_v, lasts_v, codes,
                 lasts, weight, bias, result, panels, partials, boxes, gather_sems, reduce_sems,
                 local_sems, tile_sems, out_sems):
    sub_tiles = features.shape[0]
    tile_size, width = panels[0].shape[1:]
    slot_count = tiles_hbm.shape[2]
    lanes = len(panels)
    me_row, me_col = lax.axis_index("row"), lax.axis_index("col")

    def local(number, src, dst):
        return pltpu.make_async_copy(src, dst, local_sems.at[number])

    owns = []
    for lane in range(lanes):
        owns.append(local(lane, features.at[:, :, pl.ds(lane * width, width)],
                          panels[lane].at[pl.ds(me_row * sub_tiles, sub_tiles)]))
    small = [local(lanes, tile_rows, rows_v), local(lanes + 1, tile_cols, cols_v),
             local(lanes + 2, valid, valid_v)]
    params = [local(lanes + 3, weight_hbm, weight), local(lanes + 4, bias_hbm, bias)]
    share = slot_count // TILE_COPIES
    loads = []
    for k in range(TILE_COPIES):
        part = pl.ds(k * share, share)
        loads.append(pltpu.make_async_copy(
            tiles_hbm.at[0, 0, part], tiles.at[part], tile_sems.at[k]))
    for item in owns + small + params + loads:
        item.start()

    gathers = [gather_lane(panels[lane], *gather_sems[lane], sub_tiles) for lane in range(lanes)]
    reduces = [reduce_lane(prefix, lasts, partials[lane], boxes[lane], reduce_sems[lane], columns)
               for lane in range(lanes)]

    barrier = pltpu.get_barrier_semaphore()
    peers = gathers[0][0]
    for peer in peers:
        pl.semaphore_signal(barrier, inc=1, device_id={"row": peer}, device_id_type=MESH)

    @pl.when(me_col > 0)
    def _():
        pl.semaphore_signal(barrier, inc=1, device_id={"col": me_col - 1}, device_id_type=MESH)

    @pl.when(me_col < columns - 1)
    def _():
        pl.semaphore_signal(barrier, inc=1, device_id={"col": me_col + 1}, device_id_type=MESH)

    inside = jnp.logical_and(me_col > 0, me_col < columns - 1)

    @pl.when(inside)
    def _():
        pl.semaphore_wait(barrier, len(peers) + 2)

    @pl.when(jnp.logical_not(inside))
    def _():
        pl.semaphore_wait(barrier, len(peers) + 1)

    owns[0].wait()
    gathers[0][1]()
    for item in small:
        item.wait()
    wanted_order(rows_v, cols_v, valid_v, codes_v, lasts_v, pairs)
    lists = [local(lanes, codes_v, codes), local(lanes + 1, lasts_v, lasts)]
    for item in lists:
        item.start()
    tiles[slot_count] = jnp.zeros(tiles.shape[1:], tiles.dtype)
    prefix[pairs] = jnp.zeros(prefix.shape[1:], prefix.dtype)

    for lane in range(lanes):
        _, _, receive, finish, _ = gathers[lane]
        early = list(reduces[lane - 1][1]) if lane > 0 else []
        for number in range(2):
            receive(number)
        if lane + 1 < lanes:
            owns[lane + 1].wait()
            gathers[lane + 1][1]()
        for number in range(2, 6):
            if number % 2 == 0:
                for _ in range(CUTS):
                    if early:
                        early.pop(0)()
            receive(number)
        finish()
        if lane == 0:
            for item in lists + loads:
                item.wait()
        multiply(codes, tiles, panels[lane], prefix, pairs)
        reduces[lane][0]()
        for item in early:
            item()
    for item in reduces[-1][1]:
        item()
    for item in params:
        item.wait()
    tiles_each = boxes[0].shape[1]
    cut = tiles_each // CUTS
    outs = []
    for piece in range(CUTS):
        for lane in range(lanes):
            reduces[lane][2](piece)

        def body(k, carry):
            tile = piece * cut + k
            summed = jnp.concatenate(
                [partial[me_col * tiles_each + tile].astype(jnp.bfloat16) for partial in partials],
                axis=1)
            mixed = jnp.dot(summed, weight[...], preferred_element_type=jnp.float32) + bias[...]
            start = pl.multiple_of(tile * tile_size, tile_size)
            result[pl.ds(start, tile_size), :] = jnp.maximum(mixed, 0.0).astype(result.dtype)
            return carry

        lax.fori_loop(0, cut, body, 0)
        part = pl.ds(piece * cut * tile_size, cut * tile_size)
        item = pltpu.make_async_copy(result.at[part], out.at[part], out_sems.at[piece])
        item.start()
        outs.append(item)
    for lane in range(lanes):
        gathers[lane][4]()
        reduces[lane][3]()
    for item in outs:
        item.wait()


def layer(features, tiles, tile_rows, tile_cols, valid, weight, bias, rows, columns):
    sub_rows, channels = features.shape
    slot_count, tile_size = tiles.shape[2], tiles.shape[3]
    lanes = channels // LANES
    row_tiles = sub_rows * columns // tile_size
    pairs = -(-(slot_count // 2 + row_tiles) // (2 * PAIR_UNROLL)) * PAIR_UNROLL
    tiles_each = row_tiles // columns
    codes_room = -(-2 * pairs // LANES) * LANES
    vmem, smem, dma = pltpu.VMEM, pltpu.SMEM, pltpu.SemaphoreType.DMA
    copies, moves = 14, 2 * (columns - 1) * CUTS
    scratch = [
        vmem((slot_count + 1, tile_size, tile_size), jnp.bfloat16),
        vmem((pairs + 1, tile_size, LANES), jnp.float32),
        vmem(tile_rows.shape, jnp.int32), vmem(tile_cols.shape, jnp.int32), vmem(valid.shape, jnp.int32),
        vmem((1, codes_room), jnp.int32), vmem((1, LANES), jnp.int32),
        smem((1, codes_room), jnp.int32), smem((1, LANES), jnp.int32),
        vmem(weight.shape, weight.dtype), vmem((1, channels), bias.dtype),
        vmem(features.shape, jnp.bfloat16),
        [vmem((rows * tiles_each, tile_size, LANES), jnp.bfloat16)] * lanes,
        [vmem((row_tiles, tile_size, LANES), jnp.float32)] * lanes,
        [vmem((columns + 1, tiles_each, tile_size, LANES), jnp.bfloat16)] * lanes,
        [[dma((copies,))] * 2] * lanes,
        [[dma((moves,))] * 2] * lanes,
        dma((lanes + 5,)), dma((TILE_COPIES,)), dma((CUTS,)),
    ]
    hbm = pl.BlockSpec(memory_space=pl.ANY)
    return pl.pallas_call(
        functools.partial(layer_kernel, rows, columns, pairs),
        out_shape=jax.ShapeDtypeStruct(features.shape, jnp.bfloat16),
        in_specs=[hbm] * 7, out_specs=hbm, scratch_shapes=scratch,
        compiler_params=pltpu.CompilerParams(
            collective_id=0, has_side_effects=True, vmem_limit_bytes=VMEM_ROOM),
    )(features.reshape(tiles_each, tile_size, channels), tiles, tile_rows, tile_cols, valid, weight,
      bias.reshape(1, channels))


def fits(features, tiles, rows, columns):
    sub_rows, channels = features.shape
    slot_count, tile_size = tiles.shape[2], tiles.shape[3]
    if rows != 8 or channels % LANES or tile_size != LANES or slot_count % LANES or slot_count >= FIELD:
        return False
    row_tiles = sub_rows * columns // tile_size
    col_tiles = sub_rows * rows // tile_size
    tile_bytes = tile_size * tile_size * 2
    lanes = channels // LANES
    pairs = (slot_count // 2 + row_tiles) // 2 + PAIR_UNROLL
    held = slot_count + 2 * pairs + lanes * (
        col_tiles + 2 * row_tiles + (columns + 1) * row_tiles // columns)
    return row_tiles <= LANES and held * tile_bytes < VMEM_ROOM - 2 * 2**20


def on_device(features, tiles, tile_rows, tile_cols, valid, weight, bias):
    sub_rows, channels = features.shape
    tile_size = tiles.shape[3]
    rows, columns = lax.axis_size("row"), lax.axis_size("col")
    if fits(features, tiles, rows, columns):
        return layer(features, tiles, tile_rows, tile_cols, valid, weight, bias, rows, columns)
    row_tiles = sub_rows * columns // tile_size
    width = min(channels, 128)
    lanes = channels // width
    cells = (valid, tile_rows, tile_cols)
    sums, partial = [], None
    for lane in range(lanes + 1):
        results = list(exchange(
            lane, features if lane < lanes else None, lane, partial, width, tile_size, rows, columns))
        if partial is not None:
            sums.append(results.pop().reshape(sub_rows, width))
        if lane < lanes:
            panel = results[0].reshape(-1, tile_size, width)
            partial = spmm(*cells, panel, tiles, row_tiles)
    mixed = bias
    for lane in range(lanes):
        mixed = mixed + jnp.dot(sums[lane], weight[lane * width:(lane + 1) * width],
                                preferred_element_type=jnp.float32)
    return jnp.maximum(mixed, 0.0).astype(jnp.bfloat16)


def solution(mesh):
    return jax.shard_map(
        on_device,
        mesh=mesh,
        in_specs=(
            P(("row", "col"), None),
            P("row", "col", None, None, None),
            P("row", "col", None),
            P("row", "col", None),
            P("row", "col", None),
            P(),
            P(),
        ),
        out_specs=P(("row", "col"), None),
        check_vma=False,
    )
```

```python
import functools

import jax
import jax.numpy as jnp
from jax import lax
from jax.experimental import pallas as pl
from jax.experimental.pallas import tpu as pltpu
from jax.sharding import PartitionSpec as P

SLOTS = 32
UNROLL = 8


def spmm_kernel(valid, rows, cols, panel_hbm, tiles_hbm, total,
                slot_list, row_list, col_list, panel, ring, ring_sem, panel_sem):
    slot_count = valid.shape[2]
    row_tiles = total.shape[0] - 1
    panel_copy = pltpu.make_async_copy(panel_hbm, panel, panel_sem)
    panel_copy.start()

    def scan(step, count):
        for k in range(UNROLL):
            slot = step * UNROLL + k
            slot_list[count] = slot
            row_list[count] = rows[0, 0, slot]
            col_list[count] = cols[0, 0, slot]
            count = count + valid[0, 0, slot]
        return count

    count = lax.fori_loop(0, slot_count // UNROLL, scan, jnp.int32(0))
    for k in range(UNROLL):
        slot_list[count + k] = 0
        row_list[count + k] = row_tiles
        col_list[count + k] = 0
    steps = (count + UNROLL - 1) // UNROLL
    filled = steps * UNROLL

    def fetch(index):
        place = lax.rem(index, SLOTS)
        return pltpu.make_async_copy(
            tiles_hbm.at[0, 0, slot_list[index]], ring.at[place], ring_sem.at[place])

    def prime(index, carry):
        @pl.when(index < filled)
        def _():
            fetch(index).start()
        return carry

    lax.fori_loop(0, SLOTS, prime, 0)
    total[...] = jnp.zeros_like(total)
    panel_copy.wait()

    def step_body(step, carry):
        base = step * UNROLL
        for k in range(UNROLL):
            fetch(base + k).wait()
        for k in range(UNROLL):
            index = base + k
            product = jnp.dot(ring[lax.rem(index, SLOTS)], panel[col_list[index]],
                              preferred_element_type=jnp.float32)
            row = row_list[index]
            total[row] = total[row] + product
        for k in range(UNROLL):
            later = base + SLOTS + k

            @pl.when(later < filled)
            def _():
                fetch(later).start()
        return carry

    lax.fori_loop(0, steps, step_body, 0)


def spmm(valid, rows, cols, panel, tiles, row_tiles):
    slot_count, tile_size = tiles.shape[2], tiles.shape[3]
    width = panel.shape[2]
    smem = pl.BlockSpec(memory_space=pltpu.SMEM)
    hbm = pl.BlockSpec(memory_space=pl.ANY)
    return pl.pallas_call(
        spmm_kernel,
        out_shape=jax.ShapeDtypeStruct((row_tiles + 1, tile_size, width), jnp.float32),
        in_specs=[smem, smem, smem, hbm, hbm],
        out_specs=pl.BlockSpec(memory_space=pltpu.VMEM),
        scratch_shapes=[
            pltpu.SMEM((slot_count + UNROLL,), jnp.int32),
            pltpu.SMEM((slot_count + UNROLL,), jnp.int32),
            pltpu.SMEM((slot_count + UNROLL,), jnp.int32),
            pltpu.VMEM(panel.shape, jnp.bfloat16),
            pltpu.VMEM((SLOTS, tile_size, tile_size), jnp.bfloat16),
            pltpu.SemaphoreType.DMA((SLOTS,)),
            pltpu.SemaphoreType.DMA,
        ],
        compiler_params=pltpu.CompilerParams(vmem_limit_bytes=60 * 2**20),
        cost_estimate=pl.CostEstimate(
            flops=slot_count * tile_size * tile_size * width, bytes_accessed=32 * 2**20,
            transcendentals=0),
    )(valid, rows, cols, panel, tiles)


MESH = pl.DeviceIdType.MESH
PIECES = 2


def gather_steps(features, lane, panel, send_sem, recv_sem, local_sem, rows):
    sub_rows, width = panel.shape[1], panel.shape[2]
    cut = sub_rows // 2
    me = lax.axis_index("row")
    chips = rows // 2
    core, chip = lax.rem(me, 2), me // 2
    partner = chip * 2 + (1 - core)
    own = features.at[:, pl.ds(lane * width, width)]

    def half(ref, k):
        return ref.at[pl.ds(k * cut, cut)]

    def copy(src, block, k, number, target):
        return pltpu.make_async_remote_copy(
            src_ref=src, dst_ref=half(panel.at[block], k), send_sem=send_sem.at[number],
            recv_sem=recv_sem.at[number], device_id={"row": target}, device_id_type=MESH)

    def held(block, k):
        return half(panel.at[block], k)

    if chips == 4:
        over_x, over_y = lax.rem(chip, 2), chip // 2
        x_side = (over_y * 2 + (1 - over_x)) * 2 + core
        y_side = ((1 - over_y) * 2 + over_x) * 2 + core
        across = ((1 - over_y) * 2 + (1 - over_x)) * 2 + core
        peers = [x_side, y_side]
        sources = [x_side, y_side, y_side, x_side]
        own_copies = [copy(half(own, 0), me, 0, 0, x_side), copy(half(own, 1), me, 1, 1, y_side),
                      copy(half(own, 1), me, 1, 2, x_side), copy(half(own, 0), me, 0, 3, y_side)]
        passed = {0: copy(held(x_side, 0), x_side, 0, 4, y_side),
                  1: copy(held(y_side, 1), y_side, 1, 5, x_side)}
        arriving = [(x_side, 0), (y_side, 1), (x_side, 1), (y_side, 0), (across, 0), (across, 1)]
    else:
        peers = [lax.rem(chip + k, chips) * 2 + core for k in range(1, chips)]
        from_peers = [lax.rem(chip + chips - k, chips) * 2 + core for k in range(1, chips)]
        own_copies, passed, arriving = [], {}, []
        for place, (peer, giver) in enumerate(zip(peers, from_peers)):
            for k in range(2):
                own_copies.append(copy(half(own, k), me, k, 2 * place + k, peer))
                arriving.append((giver, k))
    direct = len(arriving)
    started = list(own_copies)
    keep = pltpu.make_async_copy(own, panel.at[me], local_sem)

    def begin():
        for item in own_copies:
            item.start()
        for k in range(2):
            item = copy(half(own, k), me, k, direct + k, partner)
            item.start()
            started.append(item)
        keep.start()

    def receive(number):
        block, k = arriving[number]
        copy(held(block, k), block, k, number, partner).wait_recv()
        if number in passed:
            passed[number].start()
            started.append(passed[number])
        item = copy(held(block, k), block, k, direct + 2 + number, partner)
        item.start()
        started.append(item)

    def finish():
        for number in range(direct + 2):
            copy(held(me, 0), me, 0, direct + number, partner).wait_recv()
        for item in started:
            item.wait_send()
        keep.wait()

    steps = [functools.partial(receive, number) for number in range(direct)]
    return peers + [partner], begin, steps, finish


def reduce_steps(partial, summed, to_right, to_left, from_left, from_right, total, sems, columns):
    tiles_each = summed.shape[0]
    cut = tiles_each // PIECES
    me = lax.axis_index("col")
    right_send, right_recv, left_send, left_recv = sems

    def move(rightward, dest, piece):
        place = dest - 1 if rightward else dest
        outbox, inbox = (to_right, from_left) if rightward else (to_left, from_right)
        send, recv = (right_send, right_recv) if rightward else (left_send, left_recv)
        part = pl.ds(piece * cut, cut)
        inner = (me < dest) if rightward else (me > dest)
        first = (me == 0) if rightward else (me == columns - 1)
        number = place * PIECES + piece
        target = me + 1 if rightward else me - 1
        item = pltpu.make_async_remote_copy(
            src_ref=outbox.at[place, part], dst_ref=inbox.at[place, part],
            send_sem=send.at[number], recv_sem=recv.at[number],
            device_id={"col": target}, device_id_type=MESH)
        here = pl.ds(dest * tiles_each + piece * cut, cut)

        def open_chain():
            @pl.when(first)
            def _():
                outbox[place, part] = partial[here].astype(outbox.dtype)
                item.start()

        def pass_on():
            @pl.when(jnp.logical_and(inner, jnp.logical_not(first)))
            def _():
                item.wait_recv()
                outbox[place, part] = (
                    partial[here] + inbox[place, part].astype(jnp.float32)).astype(outbox.dtype)
                item.start()

        def close_chain():
            @pl.when(me == dest)
            def _():
                item.wait_recv()
                total[part] = total[part] + inbox[place, part].astype(jnp.float32)

        def drain():
            @pl.when(inner)
            def _():
                item.wait_send()

        return open_chain, pass_on, close_chain, drain

    links = []
    for turn in range(columns - 1):
        for piece in range(PIECES):
            links.append(move(True, columns - 1 - turn, piece))
            links.append(move(False, turn, piece))

    def begin():
        for link in links:
            link[0]()
        total[...] = partial[pl.ds(me * tiles_each, tiles_each)]

    def finish():
        for link in links:
            link[2]()
        summed[...] = total[...].astype(summed.dtype)
        for link in links:
            link[3]()

    return begin, [link[1] for link in links], finish


def exchange_kernel(gathering, reducing, lane, rows, columns, *refs):
    refs = list(refs)
    features = refs.pop(0) if gathering else None
    partial = refs.pop(0) if reducing else None
    panel = refs.pop(0) if gathering else None
    summed = refs.pop(0) if reducing else None
    peers, queue = [], []
    if gathering:
        send_sem, recv_sem, local_sem = refs.pop(0), refs.pop(0), refs.pop(0)
        peers, gather_begin, gather_list, gather_finish = gather_steps(
            features, lane, panel, send_sem, recv_sem, local_sem, rows)
    if reducing:
        reduce_begin, reduce_list, reduce_finish = reduce_steps(
            partial, summed, *refs[:5], refs[5:9], columns)

    barrier = pltpu.get_barrier_semaphore()
    for peer in peers:
        pl.semaphore_signal(barrier, inc=1, device_id={"row": peer}, device_id_type=MESH)
    expected = len(peers)
    if reducing:
        me = lax.axis_index("col")

        @pl.when(me > 0)
        def _():
            pl.semaphore_signal(barrier, inc=1, device_id={"col": me - 1}, device_id_type=MESH)

        @pl.when(me < columns - 1)
        def _():
            pl.semaphore_signal(barrier, inc=1, device_id={"col": me + 1}, device_id_type=MESH)

        inside = jnp.logical_and(me > 0, me < columns - 1)

        @pl.when(inside)
        def _():
            pl.semaphore_wait(barrier, expected + 2)

        @pl.when(jnp.logical_not(inside))
        def _():
            pl.semaphore_wait(barrier, expected + 1)
    else:
        pl.semaphore_wait(barrier, expected)

    if gathering:
        gather_begin()
    if reducing:
        reduce_begin()
    gather_queue = list(gather_list) if gathering else []
    reduce_queue = list(reduce_list) if reducing else []
    while gather_queue or reduce_queue:
        for queue in (gather_queue, reduce_queue):
            for _ in range(2):
                if queue:
                    queue.pop(0)()
    if gathering:
        gather_finish()
    if reducing:
        reduce_finish()


def exchange(number, features, lane, partial, width, tile_size, rows, columns):
    gathering, reducing = features is not None, partial is not None
    hbm, vmem = pl.BlockSpec(memory_space=pl.ANY), pl.BlockSpec(memory_space=pltpu.VMEM)
    operands, in_specs, out_shape, out_specs, scratch = [], [], [], [], []
    if gathering:
        sub_rows = features.shape[0]
        operands.append(features)
        in_specs.append(hbm)
        out_shape.append(jax.ShapeDtypeStruct((rows, sub_rows, width), jnp.bfloat16))
        out_specs.append(hbm)
        chips = rows // 2
        copies = 2 * (6 if chips == 4 else 2 * (chips - 1)) + 2
        scratch += [pltpu.SemaphoreType.DMA((copies,)), pltpu.SemaphoreType.DMA((copies,)),
                    pltpu.SemaphoreType.DMA]
    if reducing:
        tiles_each = (partial.shape[0] - 1) // columns
        operands.append(partial)
        in_specs.append(vmem)
        out_shape.append(jax.ShapeDtypeStruct((tiles_each, tile_size, width), jnp.bfloat16))
        out_specs.append(vmem)
        scratch += [pltpu.VMEM((columns - 1, tiles_each, tile_size, width), jnp.bfloat16)] * 4
        scratch += [pltpu.VMEM((tiles_each, tile_size, width), jnp.float32)]
        scratch += [pltpu.SemaphoreType.DMA(((columns - 1) * PIECES,))] * 4
    return pl.pallas_call(
        functools.partial(exchange_kernel, gathering, reducing, lane, rows, columns),
        out_shape=out_shape, in_specs=in_specs, out_specs=out_specs, scratch_shapes=scratch,
        compiler_params=pltpu.CompilerParams(
            collective_id=number, has_side_effects=True, vmem_limit_bytes=60 * 2**20),
    )(*operands)


LANES = 128
FIELD_BITS = 10
FIELD = 2**FIELD_BITS
FIRST = FIELD * FIELD
PAIR_UNROLL = 16
CUTS = 4
TILE_COPIES = 8
VMEM_ROOM = 63 * 2**20
TILE_TIME, HOP_TIME, PRODUCT_TIME, ENTRY_TIME = 0.7, 1.8, 6.0, 3.0


def group_widths(channels):
    half = LANES // 2
    return (half, half) + (LANES,) * ((channels - LANES) // LANES)


def wanted_order(rows_v, cols_v, valid_v, codes_v, lasts_v, pairs):
    slot_count = rows_v.shape[2]
    lane = lax.broadcasted_iota(jnp.int32, (1, LANES), 1)
    tall = lax.broadcasted_iota(jnp.int32, (LANES, LANES), 0)
    tall_slots = lax.broadcasted_iota(jnp.int32, (slot_count, LANES), 0)
    chunks = slot_count // LANES

    def upright(pieces):
        turned = [jnp.broadcast_to(piece, (LANES, LANES)).T for piece in pieces]
        return turned[0] if len(turned) == 1 else jnp.concatenate(turned, axis=0)

    def tally(hits, amounts):
        return jnp.sum(jnp.where(hits, amounts, 0), axis=0, keepdims=True)

    keys, columns_of = [], []
    for chunk in range(chunks):
        part = pl.ds(chunk * LANES, LANES)
        keys.append(jnp.where(valid_v[0, :, part] > 0, rows_v[0, :, part], -1))
        columns_of.append(cols_v[0, :, part])
    key_tall = upright(keys)
    held = tally(key_tall == lane, 1)
    halves = lax.shift_right_logical(held + 1, 1)
    halves_tall = upright([halves])
    lasts_v[...] = jnp.where(
        held > 0, tally(tall < lane, halves_tall) + halves - 1, pairs)
    places, codes = [], []
    for chunk in range(chunks):
        slot = lane + chunk * LANES
        before = tally(jnp.logical_and(key_tall == keys[chunk], tall_slots < slot), 1)
        start = tally(tall < keys[chunk], halves_tall)
        places.append(jnp.where(keys[chunk] >= 0, 2 * start + before, -1))
        codes.append(slot - slot_count + columns_of[chunk] * FIELD
                     + jnp.where(before == 0, FIRST, 0))
    place_tall, code_tall = upright(places), upright(codes)
    for chunk in range(codes_v.shape[1] // LANES):
        found = tally(place_tall == lane + chunk * LANES, code_tall)
        codes_v[:, pl.ds(chunk * LANES, LANES)] = found + slot_count


def pack_own(own, panel, place, sub_tiles, width, channel):
    packed = LANES // width
    each = sub_tiles // packed
    lane = lax.broadcasted_iota(jnp.int32, own.shape[1:2] + (LANES,), 1)
    chunk, offset = channel // LANES, channel % LANES

    def body(k, carry):
        value = None
        for h in range(packed):
            piece = own[h * each + k, :, pl.ds(chunk * LANES, LANES)].astype(jnp.float32)
            turn = (h * width - offset) % LANES
            piece = pltpu.roll(piece, turn, 1) if turn else piece
            value = piece if value is None else jnp.where(lane >= h * width, piece, value)
        panel[place + k] = value.astype(panel.dtype)
        return carry

    lax.fori_loop(0, each, body, 0)


def multiply(codes, tiles, panel, prefix, masks, pairs, sub_tiles):
    packed = masks.shape[0] if masks is not None else 1
    each = sub_tiles // packed

    def operands(code):
        column = jnp.bitwise_and(lax.shift_right_logical(code, FIELD_BITS), FIELD - 1)
        tile = tiles[jnp.bitwise_and(code, FIELD - 1)]
        if packed == 1:
            return tile, panel[column]
        bits = each.bit_length() - 1
        upper = lax.shift_right_logical(column, bits)
        block = lax.shift_right_logical(upper, packed.bit_length() - 1)
        share = jnp.bitwise_and(upper, packed - 1)
        value = panel[block * each + jnp.bitwise_and(column, each - 1)]
        return tile, value * masks[share]

    def body(step, total):
        for k in range(PAIR_UNROLL):
            pair = step * PAIR_UNROLL + k
            code = codes[0, 2 * pair]
            left, upper = operands(code)
            right, lower = operands(codes[0, 2 * pair + 1])
            product = jnp.dot(jnp.concatenate([left, right], axis=1),
                              jnp.concatenate([upper, lower], axis=0),
                              preferred_element_type=jnp.float32)
            opens = jnp.full(total.shape, code, jnp.int32) >= FIRST
            total = jnp.where(opens, 0.0, total) + product
            prefix[pair] = total
        return total

    lax.fori_loop(0, pairs // PAIR_UNROLL, body, jnp.zeros(panel.shape[1:], jnp.float32))


def gather_group(panel, send_sem, recv_sem, each):
    cut = each // 2
    me = lax.axis_index("row")
    core, chip = lax.rem(me, 2), me // 2
    partner = chip * 2 + (1 - core)
    over_x, over_y = lax.rem(chip, 2), chip // 2
    x_side = (over_y * 2 + (1 - over_x)) * 2 + core
    y_side = ((1 - over_y) * 2 + over_x) * 2 + core
    across = ((1 - over_y) * 2 + (1 - over_x)) * 2 + core

    def copy(block, k, number, target):
        part = panel.at[pl.ds(block * each + k * cut, cut)]
        return pltpu.make_async_remote_copy(
            src_ref=part, dst_ref=part, send_sem=send_sem.at[number],
            recv_sem=recv_sem.at[number], device_id={"row": target}, device_id_type=MESH)

    own = [(me, 0, 0, x_side), (me, 1, 1, y_side), (me, 1, 2, x_side), (me, 0, 3, y_side)]
    passed = {0: (x_side, 0, 4, y_side), 1: (y_side, 1, 5, x_side)}
    arriving = [(x_side, 0), (y_side, 1), (x_side, 1), (y_side, 0), (across, 0), (across, 1)]
    direct = len(arriving)
    started = []

    def start(*move):
        item = copy(*move)
        item.start()
        started.append(item)

    def begin():
        for move in own:
            start(*move)
        for k in range(2):
            start(me, k, direct + k, partner)

    def receive(number):
        block, k = arriving[number]
        copy(block, k, number, partner).wait_recv()
        if number in passed:
            start(*passed[number])
        start(block, k, direct + 2 + number, partner)

    def finish():
        for number in range(direct + 2):
            copy(me, 0, direct + number, partner).wait_recv()

    def drain():
        for item in started:
            item.wait_send()

    return [x_side, y_side, partner], begin, receive, finish, drain


def reduce_group(me, prefix, lasts, partial, boxes, sems, columns, packed, start):
    each = boxes.shape[1]
    cut = each // CUTS
    row_tiles = each * packed
    send, recv = sems
    last = columns - 1
    lane = lax.broadcasted_iota(jnp.int32, boxes.shape[2:], 1)
    width = LANES // packed

    def picked(dest, k):
        values = [prefix[lasts[0, dest * row_tiles + h * each + k]] for h in range(packed)]
        if packed == 1:
            return values[0]
        total = None
        for turn in range(packed):
            mixed = values[turn % packed]
            for group in range(1, packed):
                mixed = jnp.where(lane >= group * width, values[(group + turn) % packed], mixed)
            mixed = pltpu.roll(mixed, turn * width, 1) if turn else mixed
            total = mixed if total is None else total + mixed
        return total

    def each_tile(body):
        def step(k, carry):
            body(k)
            return carry
        return step

    def copy(rightward, dest, piece):
        part = pl.ds(piece * cut, cut)
        place = dest - 1 if rightward else dest
        number = ((0 if rightward else 1) * last + place) * CUTS + piece
        here = dest - me if rightward else columns - me + dest
        there = here - 1 if rightward else here + 1
        ahead = 1 if rightward else -1
        away = lambda: pltpu.make_async_remote_copy(
            src_ref=boxes.at[here, part], dst_ref=boxes.at[there, part],
            send_sem=send.at[number], recv_sem=recv.at[number],
            device_id={"col": lax.axis_index("col") + ahead}, device_id_type=MESH)
        home = lambda: pltpu.make_async_remote_copy(
            src_ref=boxes.at[here, part], dst_ref=boxes.at[here, part],
            send_sem=send.at[number], recv_sem=recv.at[number],
            device_id={"col": lax.axis_index("col") + ahead}, device_id_type=MESH)
        return here, away, home

    sent = []

    def open_chain(rightward, dest, piece):
        here, away, _ = copy(rightward, dest, piece)

        def body(k):
            boxes[here, k] = picked(dest, k).astype(boxes.dtype)
        lax.fori_loop(piece * cut, (piece + 1) * cut, each_tile(body), 0)
        away().start()
        sent.append(away)

    def pass_on(rightward, dest, piece):
        here, away, home = copy(rightward, dest, piece)
        home().wait_recv()

        def body(k):
            boxes[here, k] = (partial[dest * each + k]
                              + boxes[here, k].astype(jnp.float32)).astype(boxes.dtype)
        lax.fori_loop(piece * cut, (piece + 1) * cut, each_tile(body), 0)
        away().start()
        sent.append(away)

    def close_chain(rightward, piece):
        here, _, home = copy(rightward, me, piece)
        home().wait_recv()

        def body(k):
            partial[me * each + k] = partial[me * each + k] + boxes[here, k].astype(jnp.float32)
        lax.fori_loop(piece * cut, (piece + 1) * cut, each_tile(body), 0)

    def keep(dest):
        def body(k):
            partial[dest * each + k] = picked(dest, k)
        lax.fori_loop(0, each, each_tile(body), 0)

    def begin():
        for turn in range(last):
            for piece in range(CUTS):
                if me == 0:
                    open_chain(True, last - turn, piece)
                if me == last:
                    open_chain(False, turn, piece)
        for dest in range(columns):
            if dest == me or 0 < me < last:
                keep(dest)

    def arrival(rightward, dest, piece):
        ahead = ((last - dest if rightward else dest) * CUTS + piece) * cut * TILE_TIME
        hops = me if rightward else last - me
        return start + ahead + hops * (cut * TILE_TIME + HOP_TIME)

    events = []
    for dest in range(columns):
        for piece in range(CUTS):
            for rightward in (True, False):
                reached = (0 < me <= dest) if rightward else (dest <= me < last)
                if not reached:
                    continue
                if dest == me:
                    action = functools.partial(close_chain, rightward, piece)
                else:
                    action = functools.partial(pass_on, rightward, dest, piece)
                events.append((arrival(rightward, dest, piece), dest == me, piece, action))

    def drain():
        for away in sent:
            away().wait_send()

    return begin, events, drain


def layer_kernel(rows, columns, pairs, widths, features, tiles_hbm, tile_rows, tile_cols, valid,
                 weight_hbm, bias_hbm, out, tiles, prefix, rows_v, cols_v, valid_v, codes_v, lasts_v,
                 codes, lasts, weight, bias, own, masks, result, panels, partials, boxes, gather_sems,
                 reduce_sems, local_sems, tile_sems, out_sems):
    sub_tiles, tile_size, channels = features.shape
    slot_count = tiles_hbm.shape[2]
    groups = len(widths)
    packs = [LANES // width for width in widths]
    eaches = [sub_tiles // packed for packed in packs]
    channel_of = [sum(widths[:g]) for g in range(groups)]
    me_row, me_col = lax.axis_index("row"), lax.axis_index("col")
    half = LANES // 2

    def local(number, src, dst):
        return pltpu.make_async_copy(src, dst, local_sems.at[number])

    def own_block(g):
        return pl.ds(me_row * eaches[g], eaches[g])

    own_load = local(0, features.at[:, :, pl.ds(0, LANES)], own)
    small = [local(1, tile_rows, rows_v), local(2, tile_cols, cols_v), local(3, valid, valid_v)]
    whole = {g: local(6 + g, features.at[:, :, pl.ds(channel_of[g], LANES)], panels[g].at[own_block(g)])
             for g in range(groups) if packs[g] == 1}
    for item in [own_load] + small:
        item.start()

    gathers = [gather_group(panels[g], *gather_sems[g], eaches[g]) for g in range(groups)]
    barrier = pltpu.get_barrier_semaphore()
    peers = gathers[0][0]
    for peer in peers:
        pl.semaphore_signal(barrier, inc=1, device_id={"row": peer}, device_id_type=MESH)

    @pl.when(me_col > 0)
    def _():
        pl.semaphore_signal(barrier, inc=1, device_id={"col": me_col - 1}, device_id_type=MESH)

    @pl.when(me_col < columns - 1)
    def _():
        pl.semaphore_signal(barrier, inc=1, device_id={"col": me_col + 1}, device_id_type=MESH)

    own_load.wait()
    pack_own(own, panels[0], me_row * eaches[0], sub_tiles, widths[0], channel_of[0])

    inside = jnp.logical_and(me_col > 0, me_col < columns - 1)

    @pl.when(inside)
    def _():
        pl.semaphore_wait(barrier, len(peers) + 2)

    @pl.when(jnp.logical_not(inside))
    def _():
        pl.semaphore_wait(barrier, len(peers) + 1)

    gathers[0][1]()
    share = slot_count // TILE_COPIES
    loads = []
    for k in range(TILE_COPIES):
        part = pl.ds(k * share, share)
        loads.append(pltpu.make_async_copy(
            tiles_hbm.at[0, 0, part], tiles.at[part], tile_sems.at[k]))
    params = [local(4, weight_hbm, weight), local(5, bias_hbm, bias)]
    for item in loads + params + list(whole.values()):
        item.start()
    for item in small:
        item.wait()
    wanted_order(rows_v, cols_v, valid_v, codes_v, lasts_v, pairs)
    lists = [local(1, codes_v, codes), local(2, lasts_v, lasts)]
    for item in lists:
        item.start()
    for g in range(1, groups):
        if packs[g] > 1:
            pack_own(own, panels[g], me_row * eaches[g], sub_tiles, widths[g], channel_of[g])
    lane = lax.broadcasted_iota(jnp.int32, masks.shape[1:], 1)
    for h in range(2):
        masks[h] = jnp.where(lax.shift_right_logical(lane, half.bit_length() - 1) == h,
                             1.0, 0.0).astype(masks.dtype)
    tiles[slot_count] = jnp.zeros(tiles.shape[1:], tiles.dtype)
    prefix[pairs] = jnp.zeros(prefix.shape[1:], prefix.dtype)

    here, links_free, starts, finishes = ENTRY_TIME + HOP_TIME, 0.0, [], []
    for g in range(groups):
        here += 3 * (eaches[g] // 2) * TILE_TIME
        finishes.append(here + HOP_TIME)
        ready = max(finishes[g], links_free if g == 0 else busy) + PRODUCT_TIME
        busy = ready
        starts.append(max(ready, links_free))
        links_free = starts[g] + (columns - 1) * eaches[g] * TILE_TIME

    def reduces_of(node):
        return [reduce_group(node, prefix, lasts, partials[g], boxes[g], reduce_sems[g], columns,
                             packs[g], starts[g]) for g in range(groups)]

    reduces = [reduces_of(node) for node in range(columns)]
    cut_rows = sub_tiles // CUTS * tile_size

    def out_copy(piece):
        part = pl.ds(piece * (sub_tiles // CUTS), sub_tiles // CUTS)
        return pltpu.make_async_copy(result.at[part], out.at[part], out_sems.at[piece])

    def mix(node, piece):
        for tile in range(piece * (sub_tiles // CUTS), (piece + 1) * (sub_tiles // CUTS)):
            mixed = bias[...]
            for g in range(groups):
                h, k = tile // eaches[g], tile % eaches[g]
                summed = partials[g][node * eaches[g] + k].astype(jnp.bfloat16)
                rows_of = weight[pl.ds(channel_of[g], widths[g]), :]
                if packs[g] > 1:
                    above = jnp.zeros((h * widths[g], channels), weight.dtype)
                    below = jnp.zeros(((packs[g] - 1 - h) * widths[g], channels), weight.dtype)
                    rows_of = jnp.concatenate(
                        [part for part in (above, rows_of, below) if part.shape[0]], axis=0)
                mixed = mixed + jnp.dot(summed, rows_of, preferred_element_type=jnp.float32)
            result[tile] = mixed.astype(result.dtype)
        out_copy(piece).start()

    waiting = []
    for node in range(columns):
        events = [event for g in range(groups) for event in reduces[node][g][1]]
        ends = {}
        for when, closing, piece, _ in reduces[node][groups - 1][1]:
            if closing:
                ends[piece] = max(when, ends.get(piece, 0.0))
        events += [(when, False, piece, functools.partial(mix, node, piece)) for piece, when in ends.items()]
        waiting.append(sorted(events, key=lambda event: event[0]))

    def serve(until):
        for node in range(columns):
            ready = [event for event in waiting[node] if event[0] <= until]
            waiting[node] = [event for event in waiting[node] if event[0] > until]
            if ready:
                @pl.when(me_col == node)
                def _():
                    for event in ready:
                        event[3]()

    here = ENTRY_TIME + HOP_TIME
    for g in range(groups):
        _, _, receive, finish, _ = gathers[g]
        for step in range(3):
            here += eaches[g] // 2 * TILE_TIME
            serve(here)
            receive(2 * step)
            receive(2 * step + 1)
            if step == 0 and g + 1 < groups:
                if g + 1 in whole:
                    whole[g + 1].wait()
                gathers[g + 1][1]()
        serve(finishes[g])
        finish()
        if g == 0:
            for item in lists + loads:
                item.wait()
        multiply(codes, tiles, panels[g], prefix, masks if packs[g] > 1 else None, pairs, sub_tiles)
        for node in range(columns):
            @pl.when(me_col == node)
            def _():
                reduces[node][g][0]()
    for item in params:
        item.wait()
    serve(float("inf"))
    for g in range(groups):
        gathers[g][4]()
    for node in range(columns):
        @pl.when(me_col == node)
        def _():
            for g in range(groups):
                reduces[node][g][2]()
    for piece in range(CUTS):
        out_copy(piece).wait()


def layer(features, tiles, tile_rows, tile_cols, valid, weight, bias, rows, columns):
    sub_rows, channels = features.shape
    slot_count, tile_size = tiles.shape[2], tiles.shape[3]
    widths = group_widths(channels)
    sub_tiles = sub_rows // tile_size
    row_tiles = sub_tiles * columns
    pairs = -(-(slot_count // 2 + row_tiles) // (2 * PAIR_UNROLL)) * PAIR_UNROLL
    codes_room = -(-2 * pairs // LANES) * LANES
    vmem, smem, dma = pltpu.VMEM, pltpu.SMEM, pltpu.SemaphoreType.DMA
    copies, moves = 14, 2 * (columns - 1) * CUTS
    eaches = [sub_tiles * width // LANES for width in widths]
    tile = (tile_size, LANES)
    scratch = [
        vmem((slot_count + 1, tile_size, tile_size), jnp.bfloat16),
        vmem((pairs + 1,) + tile, jnp.float32),
        vmem(tile_rows.shape, jnp.int32), vmem(tile_cols.shape, jnp.int32), vmem(valid.shape, jnp.int32),
        vmem((1, codes_room), jnp.int32), vmem((1, LANES), jnp.int32),
        smem((1, codes_room), jnp.int32), smem((1, LANES), jnp.int32),
        vmem(weight.shape, weight.dtype), vmem((1, channels), bias.dtype),
        vmem((sub_tiles,) + tile, jnp.bfloat16),
        vmem((2,) + tile, jnp.bfloat16),
        vmem((sub_tiles, tile_size, channels), jnp.bfloat16),
        [vmem((rows * each,) + tile, jnp.bfloat16) for each in eaches],
        [vmem((columns * each,) + tile, jnp.float32) for each in eaches],
        [vmem((columns + 1, each) + tile, jnp.bfloat16) for each in eaches],
        [[dma((copies,))] * 2 for _ in widths],
        [[dma((moves,))] * 2 for _ in widths],
        dma((len(widths) + 6,)), dma((TILE_COPIES,)), dma((CUTS,)),
    ]
    hbm = pl.BlockSpec(memory_space=pl.ANY)
    mixed = pl.pallas_call(
        functools.partial(layer_kernel, rows, columns, pairs, widths),
        out_shape=jax.ShapeDtypeStruct((sub_tiles, tile_size, channels), jnp.bfloat16),
        in_specs=[hbm] * 7, out_specs=hbm, scratch_shapes=scratch,
        compiler_params=pltpu.CompilerParams(
            collective_id=0, has_side_effects=True, vmem_limit_bytes=VMEM_ROOM),
    )(features.reshape(sub_tiles, tile_size, channels), tiles, tile_rows, tile_cols, valid, weight,
      bias.reshape(1, channels))
    return jnp.maximum(mixed, 0).reshape(sub_rows, channels)


def fits(features, tiles, rows, columns):
    sub_rows, channels = features.shape
    slot_count, tile_size = tiles.shape[2], tiles.shape[3]
    sub_tiles = sub_rows // tile_size
    if rows != 8 or channels % LANES or tile_size != LANES or slot_count % LANES or slot_count >= FIELD:
        return False
    if sub_tiles & (sub_tiles - 1) or sub_tiles < 2 * CUTS or columns < 2:
        return False
    row_tiles = sub_tiles * columns
    tile_bytes = tile_size * tile_size * 2
    pairs = (slot_count // 2 + row_tiles) // 2 + PAIR_UNROLL
    held = slot_count + 2 * pairs + channels // LANES * (
        sub_tiles * rows + 2 * row_tiles + sub_tiles * (columns + 2))
    return row_tiles <= LANES and sub_tiles * rows <= FIELD and held * tile_bytes < VMEM_ROOM - 2**20


def on_device(features, tiles, tile_rows, tile_cols, valid, weight, bias):
    sub_rows, channels = features.shape
    tile_size = tiles.shape[3]
    rows, columns = lax.axis_size("row"), lax.axis_size("col")
    if fits(features, tiles, rows, columns):
        return layer(features, tiles, tile_rows, tile_cols, valid, weight, bias, rows, columns)
    row_tiles = sub_rows * columns // tile_size
    width = min(channels, 128)
    lanes = channels // width
    cells = (valid, tile_rows, tile_cols)
    sums, partial = [], None
    for lane in range(lanes + 1):
        results = list(exchange(
            lane, features if lane < lanes else None, lane, partial, width, tile_size, rows, columns))
        if partial is not None:
            sums.append(results.pop().reshape(sub_rows, width))
        if lane < lanes:
            panel = results[0].reshape(-1, tile_size, width)
            partial = spmm(*cells, panel, tiles, row_tiles)
    mixed = bias
    for lane in range(lanes):
        mixed = mixed + jnp.dot(sums[lane], weight[lane * width:(lane + 1) * width],
                                preferred_element_type=jnp.float32)
    return jnp.maximum(mixed, 0.0).astype(jnp.bfloat16)


def solution(mesh):
    return jax.shard_map(
        on_device,
        mesh=mesh,
        in_specs=(
            P(("row", "col"), None),
            P("row", "col", None, None, None),
            P("row", "col", None),
            P("row", "col", None),
            P("row", "col", None),
            P(),
            P(),
        ),
        out_specs=P(("row", "col"), None),
        check_vma=False,
    )
```

```python
import functools

import jax
import jax.numpy as jnp
from jax import lax
from jax.experimental import pallas as pl
from jax.experimental.pallas import tpu as pltpu
from jax.sharding import PartitionSpec as P

SLOTS = 32
UNROLL = 8


def spmm_kernel(valid, rows, cols, panel_hbm, tiles_hbm, total,
                slot_list, row_list, col_list, panel, ring, ring_sem, panel_sem):
    slot_count = valid.shape[2]
    row_tiles = total.shape[0] - 1
    panel_copy = pltpu.make_async_copy(panel_hbm, panel, panel_sem)
    panel_copy.start()

    def scan(step, count):
        for k in range(UNROLL):
            slot = step * UNROLL + k
            slot_list[count] = slot
            row_list[count] = rows[0, 0, slot]
            col_list[count] = cols[0, 0, slot]
            count = count + valid[0, 0, slot]
        return count

    count = lax.fori_loop(0, slot_count // UNROLL, scan, jnp.int32(0))
    for k in range(UNROLL):
        slot_list[count + k] = 0
        row_list[count + k] = row_tiles
        col_list[count + k] = 0
    steps = (count + UNROLL - 1) // UNROLL
    filled = steps * UNROLL

    def fetch(index):
        place = lax.rem(index, SLOTS)
        return pltpu.make_async_copy(
            tiles_hbm.at[0, 0, slot_list[index]], ring.at[place], ring_sem.at[place])

    def prime(index, carry):
        @pl.when(index < filled)
        def _():
            fetch(index).start()
        return carry

    lax.fori_loop(0, SLOTS, prime, 0)
    total[...] = jnp.zeros_like(total)
    panel_copy.wait()

    def step_body(step, carry):
        base = step * UNROLL
        for k in range(UNROLL):
            fetch(base + k).wait()
        for k in range(UNROLL):
            index = base + k
            product = jnp.dot(ring[lax.rem(index, SLOTS)], panel[col_list[index]],
                              preferred_element_type=jnp.float32)
            row = row_list[index]
            total[row] = total[row] + product
        for k in range(UNROLL):
            later = base + SLOTS + k

            @pl.when(later < filled)
            def _():
                fetch(later).start()
        return carry

    lax.fori_loop(0, steps, step_body, 0)


def spmm(valid, rows, cols, panel, tiles, row_tiles):
    slot_count, tile_size = tiles.shape[2], tiles.shape[3]
    width = panel.shape[2]
    smem = pl.BlockSpec(memory_space=pltpu.SMEM)
    hbm = pl.BlockSpec(memory_space=pl.ANY)
    return pl.pallas_call(
        spmm_kernel,
        out_shape=jax.ShapeDtypeStruct((row_tiles + 1, tile_size, width), jnp.float32),
        in_specs=[smem, smem, smem, hbm, hbm],
        out_specs=pl.BlockSpec(memory_space=pltpu.VMEM),
        scratch_shapes=[
            pltpu.SMEM((slot_count + UNROLL,), jnp.int32),
            pltpu.SMEM((slot_count + UNROLL,), jnp.int32),
            pltpu.SMEM((slot_count + UNROLL,), jnp.int32),
            pltpu.VMEM(panel.shape, jnp.bfloat16),
            pltpu.VMEM((SLOTS, tile_size, tile_size), jnp.bfloat16),
            pltpu.SemaphoreType.DMA((SLOTS,)),
            pltpu.SemaphoreType.DMA,
        ],
        compiler_params=pltpu.CompilerParams(vmem_limit_bytes=60 * 2**20),
        cost_estimate=pl.CostEstimate(
            flops=slot_count * tile_size * tile_size * width, bytes_accessed=32 * 2**20,
            transcendentals=0),
    )(valid, rows, cols, panel, tiles)


MESH = pl.DeviceIdType.MESH
PIECES = 2


def gather_steps(features, lane, panel, send_sem, recv_sem, local_sem, rows):
    sub_rows, width = panel.shape[1], panel.shape[2]
    cut = sub_rows // 2
    me = lax.axis_index("row")
    chips = rows // 2
    core, chip = lax.rem(me, 2), me // 2
    partner = chip * 2 + (1 - core)
    own = features.at[:, pl.ds(lane * width, width)]

    def half(ref, k):
        return ref.at[pl.ds(k * cut, cut)]

    def copy(src, block, k, number, target):
        return pltpu.make_async_remote_copy(
            src_ref=src, dst_ref=half(panel.at[block], k), send_sem=send_sem.at[number],
            recv_sem=recv_sem.at[number], device_id={"row": target}, device_id_type=MESH)

    def held(block, k):
        return half(panel.at[block], k)

    if chips == 4:
        over_x, over_y = lax.rem(chip, 2), chip // 2
        x_side = (over_y * 2 + (1 - over_x)) * 2 + core
        y_side = ((1 - over_y) * 2 + over_x) * 2 + core
        across = ((1 - over_y) * 2 + (1 - over_x)) * 2 + core
        peers = [x_side, y_side]
        sources = [x_side, y_side, y_side, x_side]
        own_copies = [copy(half(own, 0), me, 0, 0, x_side), copy(half(own, 1), me, 1, 1, y_side),
                      copy(half(own, 1), me, 1, 2, x_side), copy(half(own, 0), me, 0, 3, y_side)]
        passed = {0: copy(held(x_side, 0), x_side, 0, 4, y_side),
                  1: copy(held(y_side, 1), y_side, 1, 5, x_side)}
        arriving = [(x_side, 0), (y_side, 1), (x_side, 1), (y_side, 0), (across, 0), (across, 1)]
    else:
        peers = [lax.rem(chip + k, chips) * 2 + core for k in range(1, chips)]
        from_peers = [lax.rem(chip + chips - k, chips) * 2 + core for k in range(1, chips)]
        own_copies, passed, arriving = [], {}, []
        for place, (peer, giver) in enumerate(zip(peers, from_peers)):
            for k in range(2):
                own_copies.append(copy(half(own, k), me, k, 2 * place + k, peer))
                arriving.append((giver, k))
    direct = len(arriving)
    started = list(own_copies)
    keep = pltpu.make_async_copy(own, panel.at[me], local_sem)

    def begin():
        for item in own_copies:
            item.start()
        for k in range(2):
            item = copy(half(own, k), me, k, direct + k, partner)
            item.start()
            started.append(item)
        keep.start()

    def receive(number):
        block, k = arriving[number]
        copy(held(block, k), block, k, number, partner).wait_recv()
        if number in passed:
            passed[number].start()
            started.append(passed[number])
        item = copy(held(block, k), block, k, direct + 2 + number, partner)
        item.start()
        started.append(item)

    def finish():
        for number in range(direct + 2):
            copy(held(me, 0), me, 0, direct + number, partner).wait_recv()
        for item in started:
            item.wait_send()
        keep.wait()

    steps = [functools.partial(receive, number) for number in range(direct)]
    return peers + [partner], begin, steps, finish


def reduce_steps(partial, summed, to_right, to_left, from_left, from_right, total, sems, columns):
    tiles_each = summed.shape[0]
    cut = tiles_each // PIECES
    me = lax.axis_index("col")
    right_send, right_recv, left_send, left_recv = sems

    def move(rightward, dest, piece):
        place = dest - 1 if rightward else dest
        outbox, inbox = (to_right, from_left) if rightward else (to_left, from_right)
        send, recv = (right_send, right_recv) if rightward else (left_send, left_recv)
        part = pl.ds(piece * cut, cut)
        inner = (me < dest) if rightward else (me > dest)
        first = (me == 0) if rightward else (me == columns - 1)
        number = place * PIECES + piece
        target = me + 1 if rightward else me - 1
        item = pltpu.make_async_remote_copy(
            src_ref=outbox.at[place, part], dst_ref=inbox.at[place, part],
            send_sem=send.at[number], recv_sem=recv.at[number],
            device_id={"col": target}, device_id_type=MESH)
        here = pl.ds(dest * tiles_each + piece * cut, cut)

        def open_chain():
            @pl.when(first)
            def _():
                outbox[place, part] = partial[here].astype(outbox.dtype)
                item.start()

        def pass_on():
            @pl.when(jnp.logical_and(inner, jnp.logical_not(first)))
            def _():
                item.wait_recv()
                outbox[place, part] = (
                    partial[here] + inbox[place, part].astype(jnp.float32)).astype(outbox.dtype)
                item.start()

        def close_chain():
            @pl.when(me == dest)
            def _():
                item.wait_recv()
                total[part] = total[part] + inbox[place, part].astype(jnp.float32)

        def drain():
            @pl.when(inner)
            def _():
                item.wait_send()

        return open_chain, pass_on, close_chain, drain

    links = []
    for turn in range(columns - 1):
        for piece in range(PIECES):
            links.append(move(True, columns - 1 - turn, piece))
            links.append(move(False, turn, piece))

    def begin():
        for link in links:
            link[0]()
        total[...] = partial[pl.ds(me * tiles_each, tiles_each)]

    def finish():
        for link in links:
            link[2]()
        summed[...] = total[...].astype(summed.dtype)
        for link in links:
            link[3]()

    return begin, [link[1] for link in links], finish


def exchange_kernel(gathering, reducing, lane, rows, columns, *refs):
    refs = list(refs)
    features = refs.pop(0) if gathering else None
    partial = refs.pop(0) if reducing else None
    panel = refs.pop(0) if gathering else None
    summed = refs.pop(0) if reducing else None
    peers, queue = [], []
    if gathering:
        send_sem, recv_sem, local_sem = refs.pop(0), refs.pop(0), refs.pop(0)
        peers, gather_begin, gather_list, gather_finish = gather_steps(
            features, lane, panel, send_sem, recv_sem, local_sem, rows)
    if reducing:
        reduce_begin, reduce_list, reduce_finish = reduce_steps(
            partial, summed, *refs[:5], refs[5:9], columns)

    barrier = pltpu.get_barrier_semaphore()
    for peer in peers:
        pl.semaphore_signal(barrier, inc=1, device_id={"row": peer}, device_id_type=MESH)
    expected = len(peers)
    if reducing:
        me = lax.axis_index("col")

        @pl.when(me > 0)
        def _():
            pl.semaphore_signal(barrier, inc=1, device_id={"col": me - 1}, device_id_type=MESH)

        @pl.when(me < columns - 1)
        def _():
            pl.semaphore_signal(barrier, inc=1, device_id={"col": me + 1}, device_id_type=MESH)

        inside = jnp.logical_and(me > 0, me < columns - 1)

        @pl.when(inside)
        def _():
            pl.semaphore_wait(barrier, expected + 2)

        @pl.when(jnp.logical_not(inside))
        def _():
            pl.semaphore_wait(barrier, expected + 1)
    else:
        pl.semaphore_wait(barrier, expected)

    if gathering:
        gather_begin()
    if reducing:
        reduce_begin()
    gather_queue = list(gather_list) if gathering else []
    reduce_queue = list(reduce_list) if reducing else []
    while gather_queue or reduce_queue:
        for queue in (gather_queue, reduce_queue):
            for _ in range(2):
                if queue:
                    queue.pop(0)()
    if gathering:
        gather_finish()
    if reducing:
        reduce_finish()


def exchange(number, features, lane, partial, width, tile_size, rows, columns):
    gathering, reducing = features is not None, partial is not None
    hbm, vmem = pl.BlockSpec(memory_space=pl.ANY), pl.BlockSpec(memory_space=pltpu.VMEM)
    operands, in_specs, out_shape, out_specs, scratch = [], [], [], [], []
    if gathering:
        sub_rows = features.shape[0]
        operands.append(features)
        in_specs.append(hbm)
        out_shape.append(jax.ShapeDtypeStruct((rows, sub_rows, width), jnp.bfloat16))
        out_specs.append(hbm)
        chips = rows // 2
        copies = 2 * (6 if chips == 4 else 2 * (chips - 1)) + 2
        scratch += [pltpu.SemaphoreType.DMA((copies,)), pltpu.SemaphoreType.DMA((copies,)),
                    pltpu.SemaphoreType.DMA]
    if reducing:
        tiles_each = (partial.shape[0] - 1) // columns
        operands.append(partial)
        in_specs.append(vmem)
        out_shape.append(jax.ShapeDtypeStruct((tiles_each, tile_size, width), jnp.bfloat16))
        out_specs.append(vmem)
        scratch += [pltpu.VMEM((columns - 1, tiles_each, tile_size, width), jnp.bfloat16)] * 4
        scratch += [pltpu.VMEM((tiles_each, tile_size, width), jnp.float32)]
        scratch += [pltpu.SemaphoreType.DMA(((columns - 1) * PIECES,))] * 4
    return pl.pallas_call(
        functools.partial(exchange_kernel, gathering, reducing, lane, rows, columns),
        out_shape=out_shape, in_specs=in_specs, out_specs=out_specs, scratch_shapes=scratch,
        compiler_params=pltpu.CompilerParams(
            collective_id=number, has_side_effects=True, vmem_limit_bytes=60 * 2**20),
    )(*operands)


LANES = 128
FIELD_BITS = 10
FIELD = 2**FIELD_BITS
FIRST = FIELD * FIELD
PAIR_UNROLL = 28
CUTS = 4
TILE_COPIES = 8
VMEM_ROOM = 63 * 2**20
PRODUCT_PARTS = 4
TILE_TIME, HOP_TIME, PRODUCT_TIME, PICK_TIME, ENTRY_TIME = 0.7, 1.8, 6.5, 1.5, 2.5


def group_widths(channels):
    first = (LANES // 4, LANES // 4, LANES // 2)
    return first + (LANES,) * ((channels - LANES) // LANES)


def wanted_order(rows_v, cols_v, valid_v, codes_v, lasts_v, pairs):
    slot_count = rows_v.shape[2]
    lane = lax.broadcasted_iota(jnp.int32, (1, LANES), 1)
    tall = lax.broadcasted_iota(jnp.int32, (LANES, LANES), 0)
    tall_slots = lax.broadcasted_iota(jnp.int32, (slot_count, LANES), 0)
    chunks = slot_count // LANES

    def upright(pieces):
        turned = [jnp.broadcast_to(piece, (LANES, LANES)).T for piece in pieces]
        return turned[0] if len(turned) == 1 else jnp.concatenate(turned, axis=0)

    def tally(hits, amounts):
        return jnp.sum(jnp.where(hits, amounts, 0), axis=0, keepdims=True)

    keys, columns_of = [], []
    for chunk in range(chunks):
        part = pl.ds(chunk * LANES, LANES)
        keys.append(jnp.where(valid_v[0, :, part] > 0, rows_v[0, :, part], -1))
        columns_of.append(cols_v[0, :, part])
    key_tall = upright(keys)
    held = tally(key_tall == lane, 1)
    halves = lax.shift_right_logical(held + 1, 1)
    halves_tall = upright([halves])
    lasts_v[...] = jnp.where(
        held > 0, tally(tall < lane, halves_tall) + halves - 1, pairs)
    places, codes = [], []
    for chunk in range(chunks):
        slot = lane + chunk * LANES
        before = tally(jnp.logical_and(key_tall == keys[chunk], tall_slots < slot), 1)
        start = tally(tall < keys[chunk], halves_tall)
        places.append(jnp.where(keys[chunk] >= 0, 2 * start + before, -1))
        codes.append(slot - slot_count + columns_of[chunk] * FIELD
                     + jnp.where(before == 0, FIRST, 0))
    place_tall, code_tall = upright(places), upright(codes)
    for chunk in range(codes_v.shape[1] // LANES):
        found = tally(place_tall == lane + chunk * LANES, code_tall)
        codes_v[:, pl.ds(chunk * LANES, LANES)] = found + slot_count


def pack_own(own, panel, place, sub_tiles, width, channel):
    packed = LANES // width
    each = sub_tiles // packed
    lane = lax.broadcasted_iota(jnp.int32, own.shape[1:2] + (LANES,), 1)
    chunk, offset = channel // LANES, channel % LANES

    def body(k, carry):
        value = None
        for h in range(packed):
            piece = own[h * each + k, :, pl.ds(chunk * LANES, LANES)].astype(jnp.float32)
            turn = (h * width - offset) % LANES
            piece = pltpu.roll(piece, turn, 1) if turn else piece
            value = piece if value is None else jnp.where(lane >= h * width, piece, value)
        panel[place + k] = value.astype(panel.dtype)
        return carry

    lax.fori_loop(0, each, body, 0)


def multiply(codes, tiles, panel, prefix, masks, first, last, total, packed, sub_tiles):
    each = sub_tiles // packed

    def operands(code):
        column = jnp.bitwise_and(lax.shift_right_logical(code, FIELD_BITS), FIELD - 1)
        tile = tiles[jnp.bitwise_and(code, FIELD - 1)]
        if packed == 1:
            return tile, panel[column]
        bits = each.bit_length() - 1
        upper = lax.shift_right_logical(column, bits)
        block = lax.shift_right_logical(upper, packed.bit_length() - 1)
        share = jnp.bitwise_and(upper, packed - 1)
        value = panel[block * each + jnp.bitwise_and(column, each - 1)]
        lane = lax.broadcasted_iota(jnp.int32, value.shape, 1)
        kept = lax.shift_right_logical(lane, (LANES // packed).bit_length() - 1) == share
        return tile, jnp.where(kept, value, 0)

    def body(step, total):
        for k in range(PAIR_UNROLL):
            pair = step * PAIR_UNROLL + k
            code = codes[0, 2 * pair]
            left, upper = operands(code)
            right, lower = operands(codes[0, 2 * pair + 1])
            product = jnp.dot(jnp.concatenate([left, right], axis=1),
                              jnp.concatenate([upper, lower], axis=0),
                              preferred_element_type=jnp.float32)
            opens = jnp.full(total.shape, code, jnp.int32) >= FIRST
            total = jnp.where(opens, 0.0, total) + product
            prefix[pair] = total
        return total

    return lax.fori_loop(first, last, body, total)


def gather_group(panel, send_sem, recv_sem, each):
    cut = each // 2
    me = lax.axis_index("row")
    core, chip = lax.rem(me, 2), me // 2
    partner = chip * 2 + (1 - core)
    over_x, over_y = lax.rem(chip, 2), chip // 2
    x_side = (over_y * 2 + (1 - over_x)) * 2 + core
    y_side = ((1 - over_y) * 2 + over_x) * 2 + core
    across = ((1 - over_y) * 2 + (1 - over_x)) * 2 + core

    def copy(block, k, number, target):
        part = panel.at[pl.ds(block * each + k * cut, cut)]
        return pltpu.make_async_remote_copy(
            src_ref=part, dst_ref=part, send_sem=send_sem.at[number],
            recv_sem=recv_sem.at[number], device_id={"row": target}, device_id_type=MESH)

    own = [(me, 0, 0, x_side), (me, 1, 1, y_side), (me, 1, 2, x_side), (me, 0, 3, y_side)]
    passed = {0: (x_side, 0, 4, y_side), 1: (y_side, 1, 5, x_side)}
    arriving = [(x_side, 0), (y_side, 1), (x_side, 1), (y_side, 0), (across, 0), (across, 1)]
    direct = len(arriving)
    started = []

    def start(*move):
        item = copy(*move)
        item.start()
        started.append(item)

    def begin():
        for move in own:
            start(*move)
        for k in range(2):
            start(me, k, direct + k, partner)

    def receive(number):
        block, k = arriving[number]
        copy(block, k, number, partner).wait_recv()
        if number in passed:
            start(*passed[number])
        start(block, k, direct + 2 + number, partner)

    def finish():
        for number in range(direct + 2):
            copy(me, 0, direct + number, partner).wait_recv()

    def drain():
        for item in started:
            item.wait_send()

    return [x_side, y_side, partner], begin, receive, finish, drain


def reduce_group(me, prefix, lasts, partial, boxes, sems, columns, packed):
    each = boxes.shape[1]
    cut = each // CUTS
    row_tiles = each * packed
    send, recv = sems
    last = columns - 1
    lane = lax.broadcasted_iota(jnp.int32, boxes.shape[2:], 1)
    width = LANES // packed

    def picked(dest, k):
        values = [prefix[lasts[0, dest * row_tiles + h * each + k]] for h in range(packed)]
        if packed == 1:
            return values[0]
        total = None
        for turn in range(packed):
            mixed = values[turn % packed]
            for group in range(1, packed):
                mixed = jnp.where(lane >= group * width, values[(group + turn) % packed], mixed)
            mixed = pltpu.roll(mixed, turn * width, 1) if turn else mixed
            total = mixed if total is None else total + mixed
        return total

    def each_tile(body):
        def step(k, carry):
            body(k)
            return carry
        return step

    def copy(rightward, dest, piece):
        part = pl.ds(piece * cut, cut)
        place = dest - 1 if rightward else dest
        number = ((0 if rightward else 1) * last + place) * CUTS + piece
        here = dest - me if rightward else columns - me + dest
        there = here - 1 if rightward else here + 1
        ahead = 1 if rightward else -1
        away = lambda: pltpu.make_async_remote_copy(
            src_ref=boxes.at[here, part], dst_ref=boxes.at[there, part],
            send_sem=send.at[number], recv_sem=recv.at[number],
            device_id={"col": lax.axis_index("col") + ahead}, device_id_type=MESH)
        home = lambda: pltpu.make_async_remote_copy(
            src_ref=boxes.at[here, part], dst_ref=boxes.at[here, part],
            send_sem=send.at[number], recv_sem=recv.at[number],
            device_id={"col": lax.axis_index("col") + ahead}, device_id_type=MESH)
        return here, away, home

    sent = []

    def open_chain(rightward, dest, piece):
        here, away, _ = copy(rightward, dest, piece)

        for k in range(piece * cut, (piece + 1) * cut):
            boxes[here, k] = picked(dest, k).astype(boxes.dtype)
        away().start()
        sent.append(away)

    def pass_on(rightward, dest, piece):
        here, away, home = copy(rightward, dest, piece)
        home().wait_recv()

        def body(k):
            boxes[here, k] = (partial[dest * each + k]
                              + boxes[here, k].astype(jnp.float32)).astype(boxes.dtype)
        lax.fori_loop(piece * cut, (piece + 1) * cut, each_tile(body), 0)
        away().start()
        sent.append(away)

    def close_chain(rightward, piece):
        here, _, home = copy(rightward, me, piece)
        home().wait_recv()

        def body(k):
            partial[me * each + k] = partial[me * each + k] + boxes[here, k].astype(jnp.float32)
        lax.fori_loop(piece * cut, (piece + 1) * cut, each_tile(body), 0)

    def keep(dest):
        def body(k):
            partial[dest * each + k] = picked(dest, k)
        lax.fori_loop(0, each, each_tile(body), 0)

    def begin():
        for turn in range(last):
            for piece in range(CUTS):
                if me == 0:
                    open_chain(True, last - turn, piece)
                if me == last:
                    open_chain(False, turn, piece)
        for dest in range(columns):
            if dest == me or 0 < me < last:
                keep(dest)

    def arrival(rightward, dest, piece):
        ahead = ((last - dest if rightward else dest) * CUTS + piece) * cut * TILE_TIME
        hops = me if rightward else last - me
        return ahead + hops * (cut * TILE_TIME + HOP_TIME)

    events = []
    for dest in range(columns):
        for piece in range(CUTS):
            for rightward in (True, False):
                reached = (0 < me <= dest) if rightward else (dest <= me < last)
                if not reached:
                    continue
                if dest == me:
                    action = functools.partial(close_chain, rightward, piece)
                else:
                    action = functools.partial(pass_on, rightward, dest, piece)
                events.append((arrival(rightward, dest, piece), dest == me, piece, action))

    def drain():
        for away in sent:
            away().wait_send()

    return begin, events, drain


def layer_kernel(rows, columns, pairs, widths, features, tiles_hbm, tile_rows, tile_cols, valid,
                 weight_hbm, bias_hbm, out, tiles, prefix, rows_v, cols_v, valid_v, codes_v, lasts_v,
                 codes, lasts, weight, bias, own, masks, result, panels, partials, boxes, gather_sems,
                 reduce_sems, local_sems, tile_sems, out_sems):
    sub_tiles, tile_size, channels = features.shape
    slot_count = tiles_hbm.shape[2]
    groups = len(widths)
    packs = [LANES // width for width in widths]
    eaches = [sub_tiles // packed for packed in packs]
    channel_of = [sum(widths[:g]) for g in range(groups)]
    me_row, me_col = lax.axis_index("row"), lax.axis_index("col")
    masks = dict(zip(sorted(set(packs) - {1}), masks))

    def local(number, src, dst):
        return pltpu.make_async_copy(src, dst, local_sems.at[number])

    def own_block(g):
        return pl.ds(me_row * eaches[g], eaches[g])

    own_load = local(0, features.at[:, :, pl.ds(0, LANES)], own)
    small = [local(1, tile_rows, rows_v), local(2, tile_cols, cols_v), local(3, valid, valid_v)]
    whole = {g: local(6 + g, features.at[:, :, pl.ds(channel_of[g], LANES)], panels[g].at[own_block(g)])
             for g in range(groups) if packs[g] == 1}
    for item in [own_load] + small:
        item.start()

    gathers = [gather_group(panels[g], *gather_sems[g], eaches[g]) for g in range(groups)]
    barrier = pltpu.get_barrier_semaphore()
    peers = gathers[0][0]
    for peer in peers:
        pl.semaphore_signal(barrier, inc=1, device_id={"row": peer}, device_id_type=MESH)

    @pl.when(me_col > 0)
    def _():
        pl.semaphore_signal(barrier, inc=1, device_id={"col": me_col - 1}, device_id_type=MESH)

    @pl.when(me_col < columns - 1)
    def _():
        pl.semaphore_signal(barrier, inc=1, device_id={"col": me_col + 1}, device_id_type=MESH)

    own_load.wait()
    pack_own(own, panels[0], me_row * eaches[0], sub_tiles, widths[0], channel_of[0])

    inside = jnp.logical_and(me_col > 0, me_col < columns - 1)

    @pl.when(inside)
    def _():
        pl.semaphore_wait(barrier, len(peers) + 2)

    @pl.when(jnp.logical_not(inside))
    def _():
        pl.semaphore_wait(barrier, len(peers) + 1)

    gathers[0][1]()
    share = slot_count // TILE_COPIES
    loads = []
    for k in range(TILE_COPIES):
        part = pl.ds(k * share, share)
        loads.append(pltpu.make_async_copy(
            tiles_hbm.at[0, 0, part], tiles.at[part], tile_sems.at[k]))
    params = [local(4, weight_hbm, weight), local(5, bias_hbm, bias)]
    for item in loads + params + list(whole.values()):
        item.start()
    for item in small:
        item.wait()
    wanted_order(rows_v, cols_v, valid_v, codes_v, lasts_v, pairs)
    lists = [local(1, codes_v, codes), local(2, lasts_v, lasts)]
    for item in lists:
        item.start()
    for g in range(1, groups):
        if packs[g] > 1:
            pack_own(own, panels[g], me_row * eaches[g], sub_tiles, widths[g], channel_of[g])
    lane = lax.broadcasted_iota(jnp.int32, tiles.shape[1:], 1)
    for packed, mask in masks.items():
        for h in range(packed):
            inside_h = jnp.logical_and(lane >= h * (LANES // packed), lane < (h + 1) * (LANES // packed))
            mask[h] = jnp.where(inside_h, 1.0, 0.0).astype(mask.dtype)
    tiles[slot_count] = jnp.zeros(tiles.shape[1:], tiles.dtype)
    prefix[pairs] = jnp.zeros(prefix.shape[1:], prefix.dtype)

    reduces = [[reduce_group(node, prefix, lasts, partials[g], boxes[g], reduce_sems[g], columns, packs[g])
                for g in range(groups)] for node in range(columns)]

    def out_copy(piece):
        part = pl.ds(piece * (sub_tiles // CUTS), sub_tiles // CUTS)
        return pltpu.make_async_copy(result.at[part], out.at[part], out_sems.at[piece])

    def mix(node, piece):
        for tile in range(piece * sub_tiles // CUTS, (piece + 1) * sub_tiles // CUTS):
            mixed = bias[...]
            for g in range(groups):
                h, k = tile // eaches[g], tile % eaches[g]
                summed = partials[g][node * eaches[g] + k].astype(jnp.bfloat16)
                rows_of = weight[pl.ds(channel_of[g], widths[g]), :]
                if packs[g] > 1:
                    above = jnp.zeros((h * widths[g], channels), weight.dtype)
                    below = jnp.zeros(((packs[g] - 1 - h) * widths[g], channels), weight.dtype)
                    rows_of = jnp.concatenate(
                        [part for part in (above, rows_of, below) if part.shape[0]], axis=0)
                mixed = mixed + jnp.dot(summed, rows_of, preferred_element_type=jnp.float32)
            result[tile] = mixed.astype(result.dtype)
        out_copy(piece).start()

    waiting, later = [[] for _ in range(columns)], [[] for _ in range(columns)]

    def expect(g, start):
        for node in range(columns):
            events = [(start + when, action) for when, closing, _, action in reduces[node][g][1]
                      if g == groups - 1 or not closing]
            later[node] += [(start + when, action) for when, closing, _, action in reduces[node][g][1]
                            if g < groups - 1 and closing]
            if g == groups - 1:
                events += [(max(when, start), action) for when, action in later[node]]
                for piece in range(CUTS):
                    when = max(when for when, closing, part, _ in reduces[node][g][1]
                               if closing and part == piece)
                    events.append((start + when + 0.01, functools.partial(mix, node, piece)))
            waiting[node] = sorted(waiting[node] + events, key=lambda event: event[0])

    def serve(until):
        for node in range(columns):
            ready = [event for event in waiting[node] if event[0] <= until]
            waiting[node] = [event for event in waiting[node] if event[0] > until]
            if ready:
                @pl.when(me_col == node)
                def _():
                    for event in ready:
                        event[1]()

    now = ENTRY_TIME
    wires, sends = now, now
    arrivals, finals = [], {}

    def begin_gather(g):
        nonlocal wires
        if g in whole:
            whole[g].wait()
        gathers[g][1]()
        cut_time = eaches[g] // 2 * TILE_TIME
        wires = max(wires, now)
        arrivals.extend([(wires + cut_time + HOP_TIME, g, 0), (wires + 2 * cut_time + HOP_TIME, g, 1)])
        wires += 2 * cut_time

    def take_arrival():
        nonlocal wires
        arrivals.sort()
        _, g, step = arrivals.pop(0)
        if step < 3:
            gathers[g][2](2 * step)
            gathers[g][2](2 * step + 1)
        if step == 0:
            cut_time = eaches[g] // 2 * TILE_TIME
            wires = max(wires, now) + cut_time
            arrivals.append((wires + HOP_TIME, g, 2))
            if g + 1 < groups:
                begin_gather(g + 1)
        if step == 2:
            arrivals.append((now + HOP_TIME, g, 3))
        if step == 3:
            gathers[g][3]()

    arrivals = [(now + (k + 1) * (eaches[0] // 2) * TILE_TIME + HOP_TIME, 0, k) for k in range(2)]
    wires += eaches[0] // 2 * TILE_TIME * 2
    finished = 0
    for g in range(groups):
        for part in range(PRODUCT_PARTS):
            while arrivals and (min(arrivals)[0] <= now or finished <= g):
                now = max(now, min(arrivals)[0])
                serve(now)
                finished += min(arrivals)[2] == 3
                take_arrival()
            serve(now)
            if g == 0 and part == 0:
                for item in lists + loads:
                    item.wait()
            steps = pairs // PAIR_UNROLL
            total = jnp.zeros(panels[g].shape[1:], jnp.float32) if part == 0 else total
            total = multiply(codes, tiles, panels[g], prefix, masks.get(packs[g]),
                             part * steps // PRODUCT_PARTS, (part + 1) * steps // PRODUCT_PARTS,
                             total, packs[g], sub_tiles)
            now += PRODUCT_TIME / PRODUCT_PARTS
        for node in range(columns):
            @pl.when(me_col == node)
            def _():
                reduces[node][g][0]()
        sends = max(sends, now)
        expect(g, sends)
        sends += (columns - 1) * eaches[g] * TILE_TIME
        now += PICK_TIME
    for item in params:
        item.wait()
    serve(float("inf"))
    for g in range(groups):
        gathers[g][4]()
    for node in range(columns):
        @pl.when(me_col == node)
        def _():
            for g in range(groups):
                reduces[node][g][2]()
    for piece in range(CUTS):
        out_copy(piece).wait()


def layer(features, tiles, tile_rows, tile_cols, valid, weight, bias, rows, columns):
    sub_rows, channels = features.shape
    slot_count, tile_size = tiles.shape[2], tiles.shape[3]
    widths = group_widths(channels)
    sub_tiles = sub_rows // tile_size
    row_tiles = sub_tiles * columns
    pairs = -(-(slot_count // 2 + row_tiles) // (2 * PAIR_UNROLL)) * PAIR_UNROLL
    codes_room = -(-2 * pairs // LANES) * LANES
    vmem, smem, dma = pltpu.VMEM, pltpu.SMEM, pltpu.SemaphoreType.DMA
    copies, moves = 14, 2 * (columns - 1) * CUTS
    eaches = [sub_tiles * width // LANES for width in widths]
    packs = sorted({LANES // width for width in widths} - {1})
    tile = (tile_size, LANES)
    scratch = [
        vmem((slot_count + 1, tile_size, tile_size), jnp.bfloat16),
        vmem((pairs + 1,) + tile, jnp.float32),
        vmem(tile_rows.shape, jnp.int32), vmem(tile_cols.shape, jnp.int32), vmem(valid.shape, jnp.int32),
        vmem((1, codes_room), jnp.int32), vmem((1, LANES), jnp.int32),
        smem((1, codes_room), jnp.int32), smem((1, LANES), jnp.int32),
        vmem(weight.shape, weight.dtype), vmem((1, channels), bias.dtype),
        vmem((sub_tiles,) + tile, jnp.bfloat16),
        [vmem((packed,) + tile, jnp.bfloat16) for packed in packs],
        vmem((sub_tiles, tile_size, channels), jnp.bfloat16),
        [vmem((rows * each,) + tile, jnp.bfloat16) for each in eaches],
        [vmem((columns * each,) + tile, jnp.float32) for each in eaches],
        [vmem((columns + 1, each) + tile, jnp.bfloat16) for each in eaches],
        [[dma((copies,))] * 2 for _ in widths],
        [[dma((moves,))] * 2 for _ in widths],
        dma((len(widths) + 6,)), dma((TILE_COPIES,)), dma((CUTS,)),
    ]
    hbm = pl.BlockSpec(memory_space=pl.ANY)
    mixed = pl.pallas_call(
        functools.partial(layer_kernel, rows, columns, pairs, widths),
        out_shape=jax.ShapeDtypeStruct((sub_tiles, tile_size, channels), jnp.bfloat16),
        in_specs=[hbm] * 7, out_specs=hbm, scratch_shapes=scratch,
        compiler_params=pltpu.CompilerParams(
            collective_id=0, has_side_effects=True, vmem_limit_bytes=VMEM_ROOM),
    )(features.reshape(sub_tiles, tile_size, channels), tiles, tile_rows, tile_cols, valid, weight,
      bias.reshape(1, channels))
    return jnp.maximum(mixed, 0).reshape(sub_rows, channels)


def fits(features, tiles, rows, columns):
    sub_rows, channels = features.shape
    slot_count, tile_size = tiles.shape[2], tiles.shape[3]
    sub_tiles = sub_rows // tile_size
    if rows != 8 or channels % LANES or tile_size != LANES or slot_count % LANES or slot_count >= FIELD:
        return False
    if sub_tiles & (sub_tiles - 1) or sub_tiles < 4 * CUTS or columns < 2:
        return False
    row_tiles = sub_tiles * columns
    tile_bytes = tile_size * tile_size * 2
    pairs = (slot_count // 2 + row_tiles) // 2 + PAIR_UNROLL
    held = slot_count + 2 * pairs + channels // LANES * (
        sub_tiles * rows + 2 * row_tiles + sub_tiles * (columns + 2))
    return row_tiles <= LANES and sub_tiles * rows <= FIELD and held * tile_bytes < VMEM_ROOM - 2**20


def on_device(features, tiles, tile_rows, tile_cols, valid, weight, bias):
    sub_rows, channels = features.shape
    tile_size = tiles.shape[3]
    rows, columns = lax.axis_size("row"), lax.axis_size("col")
    if fits(features, tiles, rows, columns):
        return layer(features, tiles, tile_rows, tile_cols, valid, weight, bias, rows, columns)
    row_tiles = sub_rows * columns // tile_size
    width = min(channels, 128)
    lanes = channels // width
    cells = (valid, tile_rows, tile_cols)
    sums, partial = [], None
    for lane in range(lanes + 1):
        results = list(exchange(
            lane, features if lane < lanes else None, lane, partial, width, tile_size, rows, columns))
        if partial is not None:
            sums.append(results.pop().reshape(sub_rows, width))
        if lane < lanes:
            panel = results[0].reshape(-1, tile_size, width)
            partial = spmm(*cells, panel, tiles, row_tiles)
    mixed = bias
    for lane in range(lanes):
        mixed = mixed + jnp.dot(sums[lane], weight[lane * width:(lane + 1) * width],
                                preferred_element_type=jnp.float32)
    return jnp.maximum(mixed, 0.0).astype(jnp.bfloat16)


def solution(mesh):
    return jax.shard_map(
        on_device,
        mesh=mesh,
        in_specs=(
            P(("row", "col"), None),
            P("row", "col", None, None, None),
            P("row", "col", None),
            P("row", "col", None),
            P("row", "col", None),
            P(),
            P(),
        ),
        out_specs=P(("row", "col"), None),
        check_vma=False,
    )
```

```python
import functools

import jax
import jax.numpy as jnp
from jax import lax
from jax.experimental import pallas as pl
from jax.experimental.pallas import tpu as pltpu
from jax.sharding import PartitionSpec as P

SLOTS = 32
UNROLL = 8


def spmm_kernel(valid, rows, cols, panel_hbm, tiles_hbm, total,
                slot_list, row_list, col_list, panel, ring, ring_sem, panel_sem):
    slot_count = valid.shape[2]
    row_tiles = total.shape[0] - 1
    panel_copy = pltpu.make_async_copy(panel_hbm, panel, panel_sem)
    panel_copy.start()

    def scan(step, count):
        for k in range(UNROLL):
            slot = step * UNROLL + k
            slot_list[count] = slot
            row_list[count] = rows[0, 0, slot]
            col_list[count] = cols[0, 0, slot]
            count = count + valid[0, 0, slot]
        return count

    count = lax.fori_loop(0, slot_count // UNROLL, scan, jnp.int32(0))
    for k in range(UNROLL):
        slot_list[count + k] = 0
        row_list[count + k] = row_tiles
        col_list[count + k] = 0
    steps = (count + UNROLL - 1) // UNROLL
    filled = steps * UNROLL

    def fetch(index):
        place = lax.rem(index, SLOTS)
        return pltpu.make_async_copy(
            tiles_hbm.at[0, 0, slot_list[index]], ring.at[place], ring_sem.at[place])

    def prime(index, carry):
        @pl.when(index < filled)
        def _():
            fetch(index).start()
        return carry

    lax.fori_loop(0, SLOTS, prime, 0)
    total[...] = jnp.zeros_like(total)
    panel_copy.wait()

    def step_body(step, carry):
        base = step * UNROLL
        for k in range(UNROLL):
            fetch(base + k).wait()
        for k in range(UNROLL):
            index = base + k
            product = jnp.dot(ring[lax.rem(index, SLOTS)], panel[col_list[index]],
                              preferred_element_type=jnp.float32)
            row = row_list[index]
            total[row] = total[row] + product
        for k in range(UNROLL):
            later = base + SLOTS + k

            @pl.when(later < filled)
            def _():
                fetch(later).start()
        return carry

    lax.fori_loop(0, steps, step_body, 0)


def spmm(valid, rows, cols, panel, tiles, row_tiles):
    slot_count, tile_size = tiles.shape[2], tiles.shape[3]
    width = panel.shape[2]
    smem = pl.BlockSpec(memory_space=pltpu.SMEM)
    hbm = pl.BlockSpec(memory_space=pl.ANY)
    return pl.pallas_call(
        spmm_kernel,
        out_shape=jax.ShapeDtypeStruct((row_tiles + 1, tile_size, width), jnp.float32),
        in_specs=[smem, smem, smem, hbm, hbm],
        out_specs=pl.BlockSpec(memory_space=pltpu.VMEM),
        scratch_shapes=[
            pltpu.SMEM((slot_count + UNROLL,), jnp.int32),
            pltpu.SMEM((slot_count + UNROLL,), jnp.int32),
            pltpu.SMEM((slot_count + UNROLL,), jnp.int32),
            pltpu.VMEM(panel.shape, jnp.bfloat16),
            pltpu.VMEM((SLOTS, tile_size, tile_size), jnp.bfloat16),
            pltpu.SemaphoreType.DMA((SLOTS,)),
            pltpu.SemaphoreType.DMA,
        ],
        compiler_params=pltpu.CompilerParams(vmem_limit_bytes=60 * 2**20),
        cost_estimate=pl.CostEstimate(
            flops=slot_count * tile_size * tile_size * width, bytes_accessed=32 * 2**20,
            transcendentals=0),
    )(valid, rows, cols, panel, tiles)


MESH = pl.DeviceIdType.MESH
PIECES = 2


def gather_steps(features, lane, panel, send_sem, recv_sem, local_sem, rows):
    sub_rows, width = panel.shape[1], panel.shape[2]
    cut = sub_rows // 2
    me = lax.axis_index("row")
    chips = rows // 2
    core, chip = lax.rem(me, 2), me // 2
    partner = chip * 2 + (1 - core)
    own = features.at[:, pl.ds(lane * width, width)]

    def half(ref, k):
        return ref.at[pl.ds(k * cut, cut)]

    def copy(src, block, k, number, target):
        return pltpu.make_async_remote_copy(
            src_ref=src, dst_ref=half(panel.at[block], k), send_sem=send_sem.at[number],
            recv_sem=recv_sem.at[number], device_id={"row": target}, device_id_type=MESH)

    def held(block, k):
        return half(panel.at[block], k)

    if chips == 4:
        over_x, over_y = lax.rem(chip, 2), chip // 2
        x_side = (over_y * 2 + (1 - over_x)) * 2 + core
        y_side = ((1 - over_y) * 2 + over_x) * 2 + core
        across = ((1 - over_y) * 2 + (1 - over_x)) * 2 + core
        peers = [x_side, y_side]
        sources = [x_side, y_side, y_side, x_side]
        own_copies = [copy(half(own, 0), me, 0, 0, x_side), copy(half(own, 1), me, 1, 1, y_side),
                      copy(half(own, 1), me, 1, 2, x_side), copy(half(own, 0), me, 0, 3, y_side)]
        passed = {0: copy(held(x_side, 0), x_side, 0, 4, y_side),
                  1: copy(held(y_side, 1), y_side, 1, 5, x_side)}
        arriving = [(x_side, 0), (y_side, 1), (x_side, 1), (y_side, 0), (across, 0), (across, 1)]
    else:
        peers = [lax.rem(chip + k, chips) * 2 + core for k in range(1, chips)]
        from_peers = [lax.rem(chip + chips - k, chips) * 2 + core for k in range(1, chips)]
        own_copies, passed, arriving = [], {}, []
        for place, (peer, giver) in enumerate(zip(peers, from_peers)):
            for k in range(2):
                own_copies.append(copy(half(own, k), me, k, 2 * place + k, peer))
                arriving.append((giver, k))
    direct = len(arriving)
    started = list(own_copies)
    keep = pltpu.make_async_copy(own, panel.at[me], local_sem)

    def begin():
        for item in own_copies:
            item.start()
        for k in range(2):
            item = copy(half(own, k), me, k, direct + k, partner)
            item.start()
            started.append(item)
        keep.start()

    def receive(number):
        block, k = arriving[number]
        copy(held(block, k), block, k, number, partner).wait_recv()
        if number in passed:
            passed[number].start()
            started.append(passed[number])
        item = copy(held(block, k), block, k, direct + 2 + number, partner)
        item.start()
        started.append(item)

    def finish():
        for number in range(direct + 2):
            copy(held(me, 0), me, 0, direct + number, partner).wait_recv()
        for item in started:
            item.wait_send()
        keep.wait()

    steps = [functools.partial(receive, number) for number in range(direct)]
    return peers + [partner], begin, steps, finish


def reduce_steps(partial, summed, to_right, to_left, from_left, from_right, total, sems, columns):
    tiles_each = summed.shape[0]
    cut = tiles_each // PIECES
    me = lax.axis_index("col")
    right_send, right_recv, left_send, left_recv = sems

    def move(rightward, dest, piece):
        place = dest - 1 if rightward else dest
        outbox, inbox = (to_right, from_left) if rightward else (to_left, from_right)
        send, recv = (right_send, right_recv) if rightward else (left_send, left_recv)
        part = pl.ds(piece * cut, cut)
        inner = (me < dest) if rightward else (me > dest)
        first = (me == 0) if rightward else (me == columns - 1)
        number = place * PIECES + piece
        target = me + 1 if rightward else me - 1
        item = pltpu.make_async_remote_copy(
            src_ref=outbox.at[place, part], dst_ref=inbox.at[place, part],
            send_sem=send.at[number], recv_sem=recv.at[number],
            device_id={"col": target}, device_id_type=MESH)
        here = pl.ds(dest * tiles_each + piece * cut, cut)

        def open_chain():
            @pl.when(first)
            def _():
                outbox[place, part] = partial[here].astype(outbox.dtype)
                item.start()

        def pass_on():
            @pl.when(jnp.logical_and(inner, jnp.logical_not(first)))
            def _():
                item.wait_recv()
                outbox[place, part] = (
                    partial[here] + inbox[place, part].astype(jnp.float32)).astype(outbox.dtype)
                item.start()

        def close_chain():
            @pl.when(me == dest)
            def _():
                item.wait_recv()
                total[part] = total[part] + inbox[place, part].astype(jnp.float32)

        def drain():
            @pl.when(inner)
            def _():
                item.wait_send()

        return open_chain, pass_on, close_chain, drain

    links = []
    for turn in range(columns - 1):
        for piece in range(PIECES):
            links.append(move(True, columns - 1 - turn, piece))
            links.append(move(False, turn, piece))

    def begin():
        for link in links:
            link[0]()
        total[...] = partial[pl.ds(me * tiles_each, tiles_each)]

    def finish():
        for link in links:
            link[2]()
        summed[...] = total[...].astype(summed.dtype)
        for link in links:
            link[3]()

    return begin, [link[1] for link in links], finish


def exchange_kernel(gathering, reducing, lane, rows, columns, *refs):
    refs = list(refs)
    features = refs.pop(0) if gathering else None
    partial = refs.pop(0) if reducing else None
    panel = refs.pop(0) if gathering else None
    summed = refs.pop(0) if reducing else None
    peers, queue = [], []
    if gathering:
        send_sem, recv_sem, local_sem = refs.pop(0), refs.pop(0), refs.pop(0)
        peers, gather_begin, gather_list, gather_finish = gather_steps(
            features, lane, panel, send_sem, recv_sem, local_sem, rows)
    if reducing:
        reduce_begin, reduce_list, reduce_finish = reduce_steps(
            partial, summed, *refs[:5], refs[5:9], columns)

    barrier = pltpu.get_barrier_semaphore()
    for peer in peers:
        pl.semaphore_signal(barrier, inc=1, device_id={"row": peer}, device_id_type=MESH)
    expected = len(peers)
    if reducing:
        me = lax.axis_index("col")

        @pl.when(me > 0)
        def _():
            pl.semaphore_signal(barrier, inc=1, device_id={"col": me - 1}, device_id_type=MESH)

        @pl.when(me < columns - 1)
        def _():
            pl.semaphore_signal(barrier, inc=1, device_id={"col": me + 1}, device_id_type=MESH)

        inside = jnp.logical_and(me > 0, me < columns - 1)

        @pl.when(inside)
        def _():
            pl.semaphore_wait(barrier, expected + 2)

        @pl.when(jnp.logical_not(inside))
        def _():
            pl.semaphore_wait(barrier, expected + 1)
    else:
        pl.semaphore_wait(barrier, expected)

    if gathering:
        gather_begin()
    if reducing:
        reduce_begin()
    gather_queue = list(gather_list) if gathering else []
    reduce_queue = list(reduce_list) if reducing else []
    while gather_queue or reduce_queue:
        for queue in (gather_queue, reduce_queue):
            for _ in range(2):
                if queue:
                    queue.pop(0)()
    if gathering:
        gather_finish()
    if reducing:
        reduce_finish()


def exchange(number, features, lane, partial, width, tile_size, rows, columns):
    gathering, reducing = features is not None, partial is not None
    hbm, vmem = pl.BlockSpec(memory_space=pl.ANY), pl.BlockSpec(memory_space=pltpu.VMEM)
    operands, in_specs, out_shape, out_specs, scratch = [], [], [], [], []
    if gathering:
        sub_rows = features.shape[0]
        operands.append(features)
        in_specs.append(hbm)
        out_shape.append(jax.ShapeDtypeStruct((rows, sub_rows, width), jnp.bfloat16))
        out_specs.append(hbm)
        chips = rows // 2
        copies = 2 * (6 if chips == 4 else 2 * (chips - 1)) + 2
        scratch += [pltpu.SemaphoreType.DMA((copies,)), pltpu.SemaphoreType.DMA((copies,)),
                    pltpu.SemaphoreType.DMA]
    if reducing:
        tiles_each = (partial.shape[0] - 1) // columns
        operands.append(partial)
        in_specs.append(vmem)
        out_shape.append(jax.ShapeDtypeStruct((tiles_each, tile_size, width), jnp.bfloat16))
        out_specs.append(vmem)
        scratch += [pltpu.VMEM((columns - 1, tiles_each, tile_size, width), jnp.bfloat16)] * 4
        scratch += [pltpu.VMEM((tiles_each, tile_size, width), jnp.float32)]
        scratch += [pltpu.SemaphoreType.DMA(((columns - 1) * PIECES,))] * 4
    return pl.pallas_call(
        functools.partial(exchange_kernel, gathering, reducing, lane, rows, columns),
        out_shape=out_shape, in_specs=in_specs, out_specs=out_specs, scratch_shapes=scratch,
        compiler_params=pltpu.CompilerParams(
            collective_id=number, has_side_effects=True, vmem_limit_bytes=60 * 2**20),
    )(*operands)


LANES = 128
FIELD_BITS = 10
FIELD = 2**FIELD_BITS
FIRST = FIELD * FIELD
PAIR_UNROLL = 56
CUTS = 4
TILE_COPIES = 8
VMEM_ROOM = 62 * 2**20
PRODUCT_PARTS = 2
TILE_TIME, HOP_TIME, PRODUCT_TIME, PICK_TIME, ENTRY_TIME, LANDING_TIME, LATER_TIME = 0.7, 1.8, 5.0, 2.5, 1.6, 3.0, 0.6


def group_widths(channels):
    first = (LANES // 4, LANES // 4, LANES // 2)
    return first + (LANES,) * ((channels - LANES) // LANES)


def wanted_order(rows_v, cols_v, valid_v, codes_v, lasts_v, pairs):
    slot_count = rows_v.shape[2]
    lane = lax.broadcasted_iota(jnp.int32, (1, LANES), 1)
    tall = lax.broadcasted_iota(jnp.int32, (LANES, LANES), 0)
    tall_slots = lax.broadcasted_iota(jnp.int32, (slot_count, LANES), 0)
    chunks = slot_count // LANES

    def upright(pieces):
        turned = [jnp.broadcast_to(piece, (LANES, LANES)).T for piece in pieces]
        return turned[0] if len(turned) == 1 else jnp.concatenate(turned, axis=0)

    def tally(hits, amounts):
        return jnp.sum(jnp.where(hits, amounts, 0), axis=0, keepdims=True)

    keys, columns_of = [], []
    for chunk in range(chunks):
        part = pl.ds(chunk * LANES, LANES)
        keys.append(jnp.where(valid_v[0, :, part] > 0, rows_v[0, :, part], -1))
        columns_of.append(cols_v[0, :, part])
    key_tall = upright(keys)
    held = tally(key_tall == lane, 1)
    halves = lax.shift_right_logical(held + 1, 1)
    halves_tall = upright([halves])
    lasts_v[...] = jnp.where(
        held > 0, tally(tall < lane, halves_tall) + halves - 1, pairs)
    places, codes = [], []
    for chunk in range(chunks):
        slot = lane + chunk * LANES
        before = tally(jnp.logical_and(key_tall == keys[chunk], tall_slots < slot), 1)
        start = tally(tall < keys[chunk], halves_tall)
        places.append(jnp.where(keys[chunk] >= 0, 2 * start + before, -1))
        codes.append(slot - slot_count + columns_of[chunk] * FIELD
                     + jnp.where(before == 0, FIRST, 0))
    place_tall, code_tall = upright(places), upright(codes)
    for chunk in range(codes_v.shape[1] // LANES):
        found = tally(place_tall == lane + chunk * LANES, code_tall)
        codes_v[:, pl.ds(chunk * LANES, LANES)] = found + slot_count


def pack_own(own, panel, place, sub_tiles, width, channel):
    packed = LANES // width
    each = sub_tiles // packed
    lane = lax.broadcasted_iota(jnp.int32, own.shape[1:2] + (LANES,), 1)
    chunk, offset = channel // LANES, channel % LANES

    def body(k, carry):
        value = None
        for h in range(packed):
            piece = own[h * each + k, :, pl.ds(chunk * LANES, LANES)].astype(jnp.float32)
            turn = (h * width - offset) % LANES
            piece = pltpu.roll(piece, turn, 1) if turn else piece
            value = piece if value is None else jnp.where(lane >= h * width, piece, value)
        panel[place + k] = value.astype(panel.dtype)
        return carry

    lax.fori_loop(0, each, body, 0)


def multiply(codes, tiles, panel, prefix, first, last, total, packed, sub_tiles):
    each = sub_tiles // packed

    def operands(code):
        column = jnp.bitwise_and(lax.shift_right_logical(code, FIELD_BITS), FIELD - 1)
        tile = tiles[jnp.bitwise_and(code, FIELD - 1)]
        if packed == 1:
            return tile, panel[column]
        bits = each.bit_length() - 1
        upper = lax.shift_right_logical(column, bits)
        block = lax.shift_right_logical(upper, packed.bit_length() - 1)
        share = jnp.bitwise_and(upper, packed - 1)
        value = panel[block * each + jnp.bitwise_and(column, each - 1)]
        lane = lax.broadcasted_iota(jnp.int32, value.shape, 1)
        kept = lax.shift_right_logical(lane, (LANES // packed).bit_length() - 1) == share
        return tile, jnp.where(kept, value, 0)

    def body(step, total):
        for k in range(PAIR_UNROLL):
            pair = step * PAIR_UNROLL + k
            code = codes[0, 2 * pair]
            left, upper = operands(code)
            right, lower = operands(codes[0, 2 * pair + 1])
            product = jnp.dot(jnp.concatenate([left, right], axis=1),
                              jnp.concatenate([upper, lower], axis=0),
                              preferred_element_type=jnp.float32)
            opens = jnp.full(total.shape, code, jnp.int32) >= FIRST
            total = jnp.where(opens, 0.0, total) + product
            prefix[pair] = total
        return total

    return lax.fori_loop(first, last, body, total)


def gather_group(panel, send_sem, recv_sem, each):
    cut = each // 2
    me = lax.axis_index("row")
    core, chip = lax.rem(me, 2), me // 2
    partner = chip * 2 + (1 - core)
    over_x, over_y = lax.rem(chip, 2), chip // 2
    x_side = (over_y * 2 + (1 - over_x)) * 2 + core
    y_side = ((1 - over_y) * 2 + over_x) * 2 + core
    across = ((1 - over_y) * 2 + (1 - over_x)) * 2 + core

    def copy(block, k, number, target):
        part = panel.at[pl.ds(block * each + k * cut, cut)]
        return pltpu.make_async_remote_copy(
            src_ref=part, dst_ref=part, send_sem=send_sem.at[number],
            recv_sem=recv_sem.at[number], device_id={"row": target}, device_id_type=MESH)

    own = [(me, 0, 0, x_side), (me, 1, 1, y_side), (me, 1, 2, x_side), (me, 0, 3, y_side)]
    passed = {0: (x_side, 0, 4, y_side), 1: (y_side, 1, 5, x_side)}
    arriving = [(x_side, 0), (y_side, 1), (x_side, 1), (y_side, 0), (across, 0), (across, 1)]
    direct = len(arriving)
    started = []

    def start(*move):
        item = copy(*move)
        item.start()
        started.append(item)

    def begin():
        for move in own:
            start(*move)
        for k in range(2):
            start(me, k, direct + k, partner)

    def receive(number):
        block, k = arriving[number]
        copy(block, k, number, partner).wait_recv()
        if number in passed:
            start(*passed[number])
        start(block, k, direct + 2 + number, partner)

    def finish():
        for number in range(direct + 2):
            copy(me, 0, direct + number, partner).wait_recv()

    def drain():
        for item in started:
            item.wait_send()

    return [x_side, y_side, partner], begin, receive, finish, drain


def reduce_group(me, prefix, lasts, partial, boxes, sems, columns, packed):
    each = boxes.shape[1]
    cut = each // CUTS
    row_tiles = each * packed
    send, recv = sems
    last = columns - 1
    lane = lax.broadcasted_iota(jnp.int32, boxes.shape[2:], 1)
    width = LANES // packed

    def picked(dest, k):
        values = [prefix[lasts[0, dest * row_tiles + h * each + k]] for h in range(packed)]
        if packed == 1:
            return values[0]
        total = None
        for turn in range(packed):
            mixed = values[turn % packed]
            for group in range(1, packed):
                mixed = jnp.where(lane >= group * width, values[(group + turn) % packed], mixed)
            mixed = pltpu.roll(mixed, turn * width, 1) if turn else mixed
            total = mixed if total is None else total + mixed
        return total

    def each_tile(body):
        def step(k, carry):
            body(k)
            return carry
        return step

    def copy(rightward, dest, piece):
        part = pl.ds(piece * cut, cut)
        place = dest - 1 if rightward else dest
        number = ((0 if rightward else 1) * last + place) * CUTS + piece
        here = dest - me if rightward else columns - me + dest
        there = here - 1 if rightward else here + 1
        ahead = 1 if rightward else -1
        away = lambda: pltpu.make_async_remote_copy(
            src_ref=boxes.at[here, part], dst_ref=boxes.at[there, part],
            send_sem=send.at[number], recv_sem=recv.at[number],
            device_id={"col": lax.axis_index("col") + ahead}, device_id_type=MESH)
        home = lambda: pltpu.make_async_remote_copy(
            src_ref=boxes.at[here, part], dst_ref=boxes.at[here, part],
            send_sem=send.at[number], recv_sem=recv.at[number],
            device_id={"col": lax.axis_index("col") + ahead}, device_id_type=MESH)
        return here, away, home

    sent = []

    def open_chain(rightward, dest, piece):
        here, away, _ = copy(rightward, dest, piece)

        for k in range(piece * cut, (piece + 1) * cut):
            boxes[here, k] = picked(dest, k).astype(boxes.dtype)
        away().start()
        sent.append(away)

    def pass_on(rightward, dest, piece):
        here, away, home = copy(rightward, dest, piece)
        home().wait_recv()

        def body(k):
            boxes[here, k] = (partial[dest * each + k]
                              + boxes[here, k].astype(jnp.float32)).astype(boxes.dtype)
        lax.fori_loop(piece * cut, (piece + 1) * cut, each_tile(body), 0)
        away().start()
        sent.append(away)

    def close_chain(rightward, piece):
        here, _, home = copy(rightward, me, piece)
        home().wait_recv()

        def body(k):
            partial[me * each + k] = partial[me * each + k] + boxes[here, k].astype(jnp.float32)
        lax.fori_loop(piece * cut, (piece + 1) * cut, each_tile(body), 0)

    def keep(dest):
        def body(k):
            partial[dest * each + k] = picked(dest, k)
        lax.fori_loop(0, each, each_tile(body), 0)

    def begin():
        for turn in range(last):
            for piece in range(CUTS):
                if me == 0:
                    open_chain(True, last - turn, piece)
                if me == last:
                    open_chain(False, turn, piece)
        for dest in range(columns):
            if dest == me or 0 < me < last:
                keep(dest)

    def arrival(rightward, dest, piece):
        ahead = ((last - dest if rightward else dest) * CUTS + piece) * cut * TILE_TIME
        hops = me if rightward else last - me
        return ahead + hops * (cut * TILE_TIME + HOP_TIME)

    events = []
    for dest in range(columns):
        for piece in range(CUTS):
            for rightward in (True, False):
                reached = (0 < me <= dest) if rightward else (dest <= me < last)
                if not reached:
                    continue
                if dest == me:
                    action = functools.partial(close_chain, rightward, piece)
                else:
                    action = functools.partial(pass_on, rightward, dest, piece)
                events.append((arrival(rightward, dest, piece), dest == me, piece, action))

    def drain():
        for away in sent:
            away().wait_send()

    return begin, events, drain


def layer_kernel(rows, columns, pairs, widths, features, tiles_hbm, tile_rows, tile_cols, valid,
                 weight_hbm, bias_hbm, out, tiles, prefix, rows_v, cols_v, valid_v, codes_v, lasts_v,
                 codes, lasts, weight, bias, own, panels, partials, boxes, gather_sems,
                 reduce_sems, local_sems, tile_sems):
    sub_tiles, tile_size, channels = features.shape
    slot_count = tiles_hbm.shape[2]
    groups = len(widths)
    packs = [LANES // width for width in widths]
    eaches = [sub_tiles // packed for packed in packs]
    channel_of = [sum(widths[:g]) for g in range(groups)]
    me_row, me_col = lax.axis_index("row"), lax.axis_index("col")

    def local(number, src, dst):
        return pltpu.make_async_copy(src, dst, local_sems.at[number])

    def own_block(g):
        return pl.ds(me_row * eaches[g], eaches[g])

    own_load = local(0, features.at[:, :, pl.ds(0, LANES)], own)
    small = [local(1, tile_rows, rows_v), local(2, tile_cols, cols_v), local(3, valid, valid_v)]
    whole = {g: local(6 + g, features.at[:, :, pl.ds(channel_of[g], LANES)], panels[g].at[own_block(g)])
             for g in range(groups) if packs[g] == 1}
    for item in [own_load] + small:
        item.start()

    gathers = [gather_group(panels[g], *gather_sems[g], eaches[g]) for g in range(groups)]
    barrier = pltpu.get_barrier_semaphore()
    peers = gathers[0][0]
    for peer in peers:
        pl.semaphore_signal(barrier, inc=1, device_id={"row": peer}, device_id_type=MESH)

    @pl.when(me_col > 0)
    def _():
        pl.semaphore_signal(barrier, inc=1, device_id={"col": me_col - 1}, device_id_type=MESH)

    @pl.when(me_col < columns - 1)
    def _():
        pl.semaphore_signal(barrier, inc=1, device_id={"col": me_col + 1}, device_id_type=MESH)

    own_load.wait()
    pack_own(own, panels[0], me_row * eaches[0], sub_tiles, widths[0], channel_of[0])

    inside = jnp.logical_and(me_col > 0, me_col < columns - 1)

    @pl.when(inside)
    def _():
        pl.semaphore_wait(barrier, len(peers) + 2)

    @pl.when(jnp.logical_not(inside))
    def _():
        pl.semaphore_wait(barrier, len(peers) + 1)

    gathers[0][1]()
    share = slot_count // TILE_COPIES
    loads = []
    for k in range(TILE_COPIES):
        part = pl.ds(k * share, share)
        loads.append(pltpu.make_async_copy(
            tiles_hbm.at[0, 0, part], tiles.at[part], tile_sems.at[k]))
    params = [local(4, weight_hbm, weight), local(5, bias_hbm, bias)]
    for item in loads + params + list(whole.values()):
        item.start()
    for item in small:
        item.wait()
    wanted_order(rows_v, cols_v, valid_v, codes_v, lasts_v, pairs)
    lists = [local(1, codes_v, codes), local(2, lasts_v, lasts)]
    for item in lists:
        item.start()
    for g in range(1, groups):
        if packs[g] > 1:
            pack_own(own, panels[g], me_row * eaches[g], sub_tiles, widths[g], channel_of[g])
    tiles[slot_count] = jnp.zeros(tiles.shape[1:], tiles.dtype)
    prefix[pairs] = jnp.zeros(prefix.shape[1:], prefix.dtype)

    reduces = [[reduce_group(node, prefix, lasts, partials[g], boxes[g], reduce_sems[g], columns, packs[g])
                for g in range(groups)] for node in range(columns)]

    def mix(node, piece):
        for tile in range(piece * sub_tiles // CUTS, (piece + 1) * sub_tiles // CUTS):
            mixed = bias[...]
            for g in range(groups):
                h, k = tile // eaches[g], tile % eaches[g]
                summed = partials[g][node * eaches[g] + k].astype(jnp.bfloat16)
                rows_of = weight[pl.ds(channel_of[g], widths[g]), :]
                if packs[g] > 1:
                    above = jnp.zeros((h * widths[g], channels), weight.dtype)
                    below = jnp.zeros(((packs[g] - 1 - h) * widths[g], channels), weight.dtype)
                    rows_of = jnp.concatenate(
                        [part for part in (above, rows_of, below) if part.shape[0]], axis=0)
                mixed = mixed + jnp.dot(summed, rows_of, preferred_element_type=jnp.float32)
            out[tile] = mixed.astype(out.dtype)

    waiting, later = [[] for _ in range(columns)], [[] for _ in range(columns)]

    def expect(g, start):
        for node in range(columns):
            events = [(start + when, action) for when, closing, _, action in reduces[node][g][1]
                      if g == groups - 1 or not closing]
            later[node] += [(start + when, action) for when, closing, _, action in reduces[node][g][1]
                            if g < groups - 1 and closing]
            if g == groups - 1:
                events += [(max(when, start), action) for when, action in later[node]]
                for piece in range(CUTS):
                    when = max(when for when, closing, part, _ in reduces[node][g][1]
                               if closing and part == piece)
                    events.append((start + when + 0.01, functools.partial(mix, node, piece)))
            waiting[node] = sorted(waiting[node] + events, key=lambda event: event[0])

    def serve(until):
        for node in range(columns):
            ready = [event for event in waiting[node] if event[0] <= until]
            waiting[node] = [event for event in waiting[node] if event[0] > until]
            if ready:
                @pl.when(me_col == node)
                def _():
                    for event in ready:
                        event[1]()

    now = ENTRY_TIME
    wires, sends = now, now
    arrivals, finals = [], {}

    def begin_gather(g):
        nonlocal wires
        if g in whole:
            whole[g].wait()
        gathers[g][1]()
        cut_time = eaches[g] // 2 * TILE_TIME
        wires = max(wires, now)
        landing = LANDING_TIME + LATER_TIME * g
        arrivals.extend([(wires + cut_time + landing, g, 0), (wires + 2 * cut_time + landing, g, 1)])
        wires += 2 * cut_time

    def take_arrival():
        nonlocal wires
        arrivals.sort()
        _, g, step = arrivals.pop(0)
        if step < 3:
            gathers[g][2](2 * step)
            gathers[g][2](2 * step + 1)
        if step == 0:
            cut_time = eaches[g] // 2 * TILE_TIME
            wires = max(wires, now) + cut_time
            arrivals.append((wires + LANDING_TIME, g, 2))
            if g + 1 < groups:
                begin_gather(g + 1)
        if step == 2:
            arrivals.append((now + HOP_TIME, g, 3))
        if step == 3:
            gathers[g][3]()

    arrivals = [(now + (k + 1) * (eaches[0] // 2) * TILE_TIME + LANDING_TIME, 0, k) for k in range(2)]
    wires += eaches[0] // 2 * TILE_TIME * 2
    finished = 0
    for g in range(groups):
        for part in range(PRODUCT_PARTS):
            while arrivals and (min(arrivals)[0] <= now or finished <= g):
                now = max(now, min(arrivals)[0])
                serve(now)
                finished += min(arrivals)[2] == 3
                take_arrival()
            serve(now)
            if g == 0 and part == 0:
                for item in lists + loads:
                    item.wait()
            steps = pairs // PAIR_UNROLL
            total = jnp.zeros(panels[g].shape[1:], jnp.float32) if part == 0 else total
            total = multiply(codes, tiles, panels[g], prefix,
                             part * steps // PRODUCT_PARTS, (part + 1) * steps // PRODUCT_PARTS,
                             total, packs[g], sub_tiles)
            now += PRODUCT_TIME / PRODUCT_PARTS
        while arrivals and min(arrivals)[0] <= now:
            finished += min(arrivals)[2] == 3
            take_arrival()
        for node in range(columns):
            @pl.when(me_col == node)
            def _():
                reduces[node][g][0]()
        sends = max(sends, now)
        expect(g, sends)
        sends += (columns - 1) * eaches[g] * TILE_TIME
        now += PICK_TIME
    for item in params:
        item.wait()
    serve(float("inf"))
    for g in range(groups):
        gathers[g][4]()
    for node in range(columns):
        @pl.when(me_col == node)
        def _():
            for g in range(groups):
                reduces[node][g][2]()


def pair_count(slot_count, row_tiles):
    return -(-(slot_count // 2 + row_tiles) // (2 * PAIR_UNROLL)) * PAIR_UNROLL


def layer(features, tiles, tile_rows, tile_cols, valid, weight, bias, rows, columns):
    sub_rows, channels = features.shape
    slot_count, tile_size = tiles.shape[2], tiles.shape[3]
    widths = group_widths(channels)
    sub_tiles = sub_rows // tile_size
    row_tiles = sub_tiles * columns
    pairs = pair_count(slot_count, row_tiles)
    codes_room = -(-2 * pairs // LANES) * LANES
    vmem, smem, dma = pltpu.VMEM, pltpu.SMEM, pltpu.SemaphoreType.DMA
    copies, moves = 14, 2 * (columns - 1) * CUTS
    eaches = [sub_tiles * width // LANES for width in widths]
    tile = (tile_size, LANES)
    scratch = [
        vmem((slot_count + 1, tile_size, tile_size), jnp.bfloat16),
        vmem((pairs + 1,) + tile, jnp.float32),
        vmem(tile_rows.shape, jnp.int32), vmem(tile_cols.shape, jnp.int32), vmem(valid.shape, jnp.int32),
        vmem((1, codes_room), jnp.int32), vmem((1, LANES), jnp.int32),
        smem((1, codes_room), jnp.int32), smem((1, LANES), jnp.int32),
        vmem(weight.shape, weight.dtype), vmem((1, channels), bias.dtype),
        vmem((sub_tiles,) + tile, jnp.bfloat16),
        [vmem((rows * each,) + tile, jnp.bfloat16) for each in eaches],
        [vmem((columns * each,) + tile, jnp.float32) for each in eaches],
        [vmem((columns + 1, each) + tile, jnp.bfloat16) for each in eaches],
        [[dma((copies,))] * 2 for _ in widths],
        [[dma((moves,))] * 2 for _ in widths],
        dma((len(widths) + 6,)), dma((TILE_COPIES,)),
    ]
    hbm = pl.BlockSpec(memory_space=pl.ANY)
    mixed = pl.pallas_call(
        functools.partial(layer_kernel, rows, columns, pairs, widths),
        out_shape=pltpu.VMEM((sub_tiles, tile_size, channels), jnp.bfloat16),
        in_specs=[hbm] * 7, out_specs=pl.BlockSpec(memory_space=pltpu.VMEM), scratch_shapes=scratch,
        compiler_params=pltpu.CompilerParams(
            collective_id=0, has_side_effects=True, vmem_limit_bytes=VMEM_ROOM),
    )(features.reshape(sub_tiles, tile_size, channels), tiles, tile_rows, tile_cols, valid, weight,
      bias.reshape(1, channels))
    return jnp.maximum(mixed, 0).reshape(sub_rows, channels)


def fits(features, tiles, rows, columns):
    sub_rows, channels = features.shape
    slot_count, tile_size = tiles.shape[2], tiles.shape[3]
    sub_tiles = sub_rows // tile_size
    if rows != 8 or channels % LANES or tile_size != LANES or slot_count % LANES or slot_count >= FIELD:
        return False
    if sub_tiles & (sub_tiles - 1) or sub_tiles < 4 * CUTS or columns < 2:
        return False
    row_tiles = sub_tiles * columns
    tile_bytes = tile_size * tile_size * 2
    pairs = pair_count(slot_count, row_tiles)
    held = slot_count + 2 * pairs + channels // LANES * (
        sub_tiles * rows + 2 * row_tiles + sub_tiles * (columns + 2))
    return row_tiles <= LANES and sub_tiles * rows <= FIELD and held * tile_bytes < VMEM_ROOM


def on_device(features, tiles, tile_rows, tile_cols, valid, weight, bias):
    sub_rows, channels = features.shape
    tile_size = tiles.shape[3]
    rows, columns = lax.axis_size("row"), lax.axis_size("col")
    if fits(features, tiles, rows, columns):
        return layer(features, tiles, tile_rows, tile_cols, valid, weight, bias, rows, columns)
    row_tiles = sub_rows * columns // tile_size
    width = min(channels, 128)
    lanes = channels // width
    cells = (valid, tile_rows, tile_cols)
    sums, partial = [], None
    for lane in range(lanes + 1):
        results = list(exchange(
            lane, features if lane < lanes else None, lane, partial, width, tile_size, rows, columns))
        if partial is not None:
            sums.append(results.pop().reshape(sub_rows, width))
        if lane < lanes:
            panel = results[0].reshape(-1, tile_size, width)
            partial = spmm(*cells, panel, tiles, row_tiles)
    mixed = bias
    for lane in range(lanes):
        mixed = mixed + jnp.dot(sums[lane], weight[lane * width:(lane + 1) * width],
                                preferred_element_type=jnp.float32)
    return jnp.maximum(mixed, 0.0).astype(jnp.bfloat16)


def solution(mesh):
    return jax.shard_map(
        on_device,
        mesh=mesh,
        in_specs=(
            P(("row", "col"), None),
            P("row", "col", None, None, None),
            P("row", "col", None),
            P("row", "col", None),
            P("row", "col", None),
            P(),
            P(),
        ),
        out_specs=P(("row", "col"), None),
        check_vma=False,
    )
```
